32 devices in a mesh: section: 4 (over z), tensor: 4 (over y, x), dp: 2 (over core).
Axes of the slice: x: 2, y: 2, z: 4, core: 2. Of those that a mesh axis runs over, the one named last changes fastest.
Arguments:
- forward_rows: bfloat16 [4, 2, 192, 8192], P('section', 'dp', None, 'tensor'), may hold values from -6 to 6
- saved_rows: bfloat16 [4, 2, 192, 8192], P('section', 'dp', None, 'tensor'), may hold values from -40.5 to 40.5
- output_grad: bfloat16 [4, 2, 192, 8192], P('section', 'dp', None, 'tensor'), may hold values from -1.27 to 1.27
- lengths: int32 [4, 2, 2], P('section', 'dp'), may hold values from 1 to 96
- norm_gain: bfloat16 [4, 8192], P('section', 'tensor'), may hold values from 0.5 to 1.5
- down_map: bfloat16 [4, 192, 8192], P('section', None, 'tensor'), may hold values from -0.067396115 to 0.067396115
- up_map: bfloat16 [4, 192, 8192], P('section', None, 'tensor'), may hold values from -1.0625 to 1.0625
Outputs:
- next_inputs: bfloat16 [4, 2, 192, 8192], P('section', 'dp', None, 'tensor')
- next_grads: bfloat16 [4, 2, 192, 8192], P('section', 'dp', None, 'tensor')
- grad_down: bfloat16 [4, 192, 8192], P('section', 'dp', 'tensor')
- grad_up: bfloat16 [4, 192, 8192], P('section', 'dp', 'tensor')
The draws below stay inside these ranges and needn't reach their ends.
All inputs are finite; a program needn't handle non-finite values.
Results may differ from the reference program's by a relative error of at most 0.02.
Values may be sent and summed in bfloat16 or wider, within the bound.
A program may use at most 64 MiB of HBM per device.

```python
import jax
import jax.numpy as jnp
from jax import lax

D = 8192
R = 192
ROWS = 192
SEQ = 96
N_SECTION = 4
N_DP = 2


def shared_rows(key):
    base = jax.random.fold_in(key, 11)
    shape = (N_SECTION, N_DP, ROWS, D)
    return jnp.clip(jax.random.normal(base, shape, jnp.float32), -6.0, 6.0)


def draw_saved_rows(key, part):
    values = shared_rows(key)
    return values.astype(jnp.bfloat16)


def draw_output_grad(key, part):
    shared = shared_rows(key)
    noise = jax.random.normal(jax.random.fold_in(key, 13), shared.shape, jnp.float32)
    mixed = 0.8 * shared + 0.6 * jnp.clip(noise, -6.0, 6.0)
    return (0.15 * mixed).astype(jnp.bfloat16)


def map_values(key, salt):
    base = jax.random.fold_in(key, salt)
    shape = (N_SECTION, R, D)
    return jnp.clip(jax.random.normal(base, shape, jnp.float32), -6.0, 6.0)


def draw_down_map(key, part):
    return (map_values(key, 21) * D ** (-0.5)).astype(jnp.bfloat16)


def draw_up_map(key, part):
    shared = map_values(key, 21)
    own_part = map_values(key, 22)
    mixed = 0.8 * shared + 0.6 * own_part
    return (mixed * (R // 3) ** (-0.5)).astype(jnp.bfloat16)


def place_ends(result, key, smallest, top_value):
    extent = result.shape
    place = [jax.random.randint(jax.random.fold_in(key, axis), (), 0, extent[axis]) for axis in range(len(extent))]
    result = result.at[tuple(place)].set(smallest)
    longest = extent.index(max(extent))
    place[longest] = (place[longest] + 1) % extent[longest]
    return result.at[tuple(place)].set(top_value)


def level_of(rng, extent, split, smallest, high):
    gain, own = 1.0, jax.random.fold_in(rng, 6)
    for dim, parts in split:
        draws = jnp.exp(jax.random.uniform(jax.random.fold_in(own, dim), (parts,), jnp.float32, smallest / len(split), high / len(split)))
        gain = gain * jnp.repeat(draws, extent[dim] // parts).reshape([-1 if axis == dim else 1 for axis in range(len(extent))])
    return gain


def normal_values(stream_key, dims, scale, most, pieces=(), held_as=jnp.bfloat16):
    factor_of = level_of(stream_key, dims, pieces, -0.22, 0.18) if pieces else 1.0
    values = jax.random.normal(stream_key, dims, jnp.float32) * scale * factor_of
    return jnp.minimum(jnp.maximum(values, -most), most).astype(held_as)


def setup_inputs(seed: int = 0) -> dict:
    seeds = jax.random.split(jax.random.key(seed), 8)
    forward_rows = normal_values(seeds[0], (N_SECTION, N_DP, ROWS, D), 1.0, 6.0, ((0, 4), (1, 2), (3, 4)))
    saved_rows = draw_saved_rows(jax.random.fold_in(seeds[7], 71), 0)
    output_grad = draw_output_grad(jax.random.fold_in(seeds[7], 71), 0)
    lengths = place_ends(jax.random.randint(seeds[3], (N_SECTION, N_DP, 2), 1, SEQ + 1), jax.random.fold_in(seeds[3], 1), 1, SEQ).astype(jnp.int32)
    norm_gain = jnp.clip(1.0 + 0.1 * jax.random.normal(seeds[4], (N_SECTION, D), jnp.float32), 0.5, 1.5).astype(jnp.bfloat16)
    down_map = draw_down_map(jax.random.fold_in(seeds[7], 71), 0)
    up_map = draw_up_map(jax.random.fold_in(seeds[7], 71), 0)
    return dict(forward_rows=forward_rows, saved_rows=saved_rows, output_grad=output_grad, lengths=lengths, norm_gain=norm_gain, down_map=down_map, up_map=up_map)


EPSILON = 1e-05

def contract_last(left_side, right_side):
    return lax.dot_general(left_side, right_side, (((1,), (1,)), ((), ())), preferred_element_type=jnp.float32)

def contract_rows(left_side, right_side):
    return lax.dot_general(left_side, right_side, (((0,), (0,)), ((), ())), preferred_element_type=jnp.float32)

def silu_slope(values):
    gate_value = jax.nn.sigmoid(values)
    return gate_value * (1.0 + values * (1.0 - gate_value))

def norm_rows(row_block, gain_cols):
    values = row_block.astype(jnp.float32)
    scale = lax.rsqrt(lax.optimization_barrier(jnp.mean(values * values, axis=1, keepdims=True)) + EPSILON)
    return (values, scale, (values * scale * gain_cols).astype(jnp.bfloat16))

def group_tick(forward_block, saved_block, incoming, seq_lengths, gain_cols, down_rows, up_rows):
    forward_values, forward_scale, forward_normed = norm_rows(forward_block, gain_cols)
    forward_act = jax.nn.silu(contract_last(forward_normed, down_rows)).astype(jnp.bfloat16)
    forward_out = (forward_values + jnp.dot(forward_act, up_rows, preferred_element_type=jnp.float32)).astype(jnp.bfloat16)
    position = jnp.arange(ROWS, dtype=jnp.int32)
    length_limit = jnp.where(position // SEQ == 0, seq_lengths[0], seq_lengths[1])
    keep_rows = position % SEQ < length_limit
    kept_grad = jnp.where(keep_rows[:, None], incoming, jnp.zeros_like(incoming))
    saved_values, saved_scale, saved_normed = norm_rows(saved_block, gain_cols)
    saved_rank = contract_last(saved_normed, down_rows)
    saved_act = jax.nn.silu(saved_rank).astype(jnp.bfloat16)
    rank_slope = contract_last(kept_grad, up_rows)
    back_rank = (rank_slope * silu_slope(saved_rank)).astype(jnp.bfloat16)
    back_normed = jnp.dot(back_rank, down_rows, preferred_element_type=jnp.float32)
    weighted = gain_cols * back_normed
    correction = lax.optimization_barrier(jnp.mean(saved_values * weighted, axis=1, keepdims=True))
    scale_cube = saved_scale * saved_scale * saved_scale
    grad_rows = (kept_grad.astype(jnp.float32) + saved_scale * weighted - saved_values * scale_cube * correction).astype(jnp.bfloat16)
    down_part = contract_rows(back_rank, saved_normed).astype(jnp.bfloat16)
    up_part = contract_rows(saved_act, kept_grad).astype(jnp.bfloat16)
    return (forward_out, grad_rows, down_part, up_part)

def section_tick(packed):
    forward_block, saved_block, incoming, seq_lengths, gain_row, down_rows, up_rows = packed
    gain_cols = gain_row.astype(jnp.float32)
    group_map = jax.vmap(group_tick, in_axes=(0, 0, 0, 0, None, None, None))
    forward_out, grad_rows, down_part, up_part = group_map(forward_block, saved_block, incoming, seq_lengths, gain_cols, down_rows, up_rows)
    down_part = lax.optimization_barrier(down_part)
    up_part = lax.optimization_barrier(up_part)
    mean_weight = 1.0 / N_DP
    grad_down = (lax.optimization_barrier(jnp.sum(down_part.astype(jnp.float32), axis=0)) * mean_weight).astype(jnp.bfloat16)
    grad_up = (lax.optimization_barrier(jnp.sum(up_part.astype(jnp.float32), axis=0)) * mean_weight).astype(jnp.bfloat16)
    return (forward_out, grad_rows, grad_down, grad_up)

def reference(forward_rows, saved_rows, output_grad, lengths, norm_gain, down_map, up_map):
    forward_out, grad_rows, grad_down, grad_up = lax.map(section_tick, (forward_rows, saved_rows, output_grad, lengths, norm_gain, down_map, up_map))
    next_inputs = jnp.concatenate([jnp.zeros_like(forward_out[:1]), forward_out[:-1]], axis=0)
    next_grads = jnp.concatenate([grad_rows[1:], jnp.zeros_like(grad_rows[:1])], axis=0)
    return (next_inputs, next_grads, grad_down, grad_up)
```

```python
import functools

import jax
import jax.numpy as jnp
from jax import lax
from jax.experimental import pallas as pl
from jax.experimental.pallas import tpu as pltpu
from jax.sharding import PartitionSpec as P

EPSILON = 1e-05
LANES = 128
RAW_FORWARD = 0.375
RAW_BACK = 0.125
F32 = jnp.float32
BF16 = jnp.bfloat16


def contract_last(left_side, right_side):
    return lax.dot_general(
        left_side, right_side, (((1,), (1,)), ((), ())), preferred_element_type=F32
    )


def contract_rows(left_side, right_side):
    return lax.dot_general(
        left_side, right_side, (((0,), (0,)), ((), ())), preferred_element_type=F32
    )


def flip(index, bit):
    step = 1 << bit
    return index + step * (1 - 2 * ((index // step) % 2))


def row_groups(rows):
    sizes = (rows // 6, rows // 3, rows // 2) if rows % 192 == 0 else (rows,)
    starts = [sum(sizes[:i]) for i in range(len(sizes))]
    return list(zip(starts, sizes))


def semaphores(n_group, bits, n_dp):
    names = ["len", "gain", "sav", "down", "grad", "up", "fwd"]
    names += [("sq", kind, p) for kind in "sr" for p in range(bits)]
    names += [("b", g, p) for g in range(n_group) for p in range(bits)] + ["b_send"]
    names += [("f", p) for p in range(bits)] + ["f_send"]
    names += [(side, kind) for side in ("out_f", "out_b") for kind in "sr"]
    names += [(side, kind) for side in ("raw_up", "raw_down", "raw_gain", "act", "back") for kind in "sr"]
    names += ["raw_fwd_r", "raw_sav_s", "raw_pair_r"]
    names += [("all", kind, p) for kind in "sr" for p in range(bits)]
    names += [("trade", kind, k) for kind in "sr" for k in range(1, n_dp)]
    names += [("relay", way, kind, k) for way in range(2) for kind in "sr" for k in range(1, n_dp)]
    return {name: i for i, name in enumerate(names)}


def tick(sizes, fwd_hbm, sav_hbm, grad_hbm, len_hbm, gain_hbm, down_hbm, up_hbm,
         next_in, next_gr, grad_down, grad_up,
         lens, gain, fwd, sav, kept, down, up, scaled,
         acc_f, acc_b, send_f, recv_f, send_b, recv_b, out_f, out_b,
         part, part_recv, act_out, back_out, pair, sq_out, sq_in,
         raw_fwd, raw_up, raw_pair, raw_down, raw_gain, sems):
    n_sec, n_ten, n_dp, chunk = sizes
    rows, width = fwd.shape
    rank = down.shape[0]
    padded = act_out.shape[1]
    full_width = width * n_ten
    n_seq = lens.shape[1]
    bits = n_ten.bit_length() - 1
    share = rank // n_dp
    quarter = rows // n_ten
    groups = row_groups(rows)
    index = semaphores(len(groups), bits, n_dp)
    sec, ten, dp = lax.axis_index("section"), lax.axis_index("tensor"), lax.axis_index("dp")

    def sem(*name):
        return sems.at[index[name if len(name) > 1 else name[0]]]

    loads = {
        name: pltpu.make_async_copy(source, target, sem(name))
        for name, source, target in (
            ("sav", sav_hbm, sav), ("gain", gain_hbm, gain), ("down", down_hbm, down), ("len", len_hbm, lens),
            ("grad", grad_hbm, kept), ("up", up_hbm, up), ("fwd", fwd_hbm, fwd),
        )
    }
    for load in loads.values():
        load.start()

    @pl.when(sec == 0)
    def _():
        pair[:, :padded] = jnp.zeros((rows, padded), BF16)

    @pl.when(sec == n_sec - 1)
    def _():
        pair[:, padded:] = jnp.zeros((rows, padded), BF16)

    barrier = pltpu.get_barrier_semaphore()
    for p in range(bits):
        pl.semaphore_signal(barrier, inc=1, device_id={"tensor": flip(ten, p)})
    for k in range(1, n_dp):
        pl.semaphore_signal(barrier, inc=1, device_id={"dp": (dp + k) % n_dp})

    @pl.when(sec > 0)
    def _():
        pl.semaphore_signal(barrier, inc=1, device_id={"section": sec - 1})

    @pl.when(sec < n_sec - 1)
    def _():
        pl.semaphore_signal(barrier, inc=1, device_id={"section": sec + 1})

    columns = [slice(c, c + chunk) for c in range(0, width, chunk)]
    raw_f, raw_b = raw_fwd.shape[1], raw_pair.shape[2]
    mine = pl.ds(pl.multiple_of(dp * share, share), share)
    own = pl.ds(pl.multiple_of(ten * quarter, quarter), quarter)
    tail_f, tail_b = pl.ds(width - raw_f, raw_f), pl.ds(width - raw_b, raw_b)

    def remote(source, target, send, recv, **place):
        return pltpu.make_async_remote_copy(
            src_ref=source, dst_ref=target, send_sem=send, recv_sem=recv, device_id=place
        )

    def across(step, source, target, send, recv):
        return remote(source, target, send, recv, section=sec + step)

    raw_ups = across(1, up.at[mine, tail_f], raw_up.at[mine], sem("raw_up", "s"), sem("raw_up", "r"))
    raw_fwds = across(1, fwd.at[:, tail_f], raw_fwd, sem("out_f", "s"), sem("raw_fwd_r"))
    acts = across(1, act_out.at[own], pair.at[own, pl.ds(0, padded)], sem("act", "s"), sem("act", "r"))
    raw_downs = across(-1, down.at[mine, tail_b], raw_down.at[mine], sem("raw_down", "s"), sem("raw_down", "r"))
    raw_gains = across(-1, gain.at[:, tail_b], raw_gain, sem("raw_gain", "s"), sem("raw_gain", "r"))
    raw_savs = across(-1, sav.at[:, tail_b], raw_pair.at[0], sem("raw_sav_s"), sem("raw_pair_r"))
    raw_keeps = across(-1, kept.at[:, tail_b], raw_pair.at[1], sem("out_b", "s"), sem("raw_pair_r"))
    raw_pairs = across(-1, raw_pair, raw_pair, sem("raw_sav_s"), sem("raw_pair_r"))
    backs = across(-1, back_out.at[own], pair.at[own, pl.ds(padded, padded)], sem("back", "s"), sem("back", "r"))

    def relay(way, k):
        ref = (raw_up, raw_down)[way].at[mine]
        return remote(ref, ref, sem("relay", way, "s", k), sem("relay", way, "r", k), dp=(dp + k) % n_dp)

    def exchange_b(start, size, g, p):
        for q in range(2):
            span = pl.ds(start + q * (size // 2), size // 2)
            remote(
                send_b.at[p, span], recv_b.at[p, span], sem("b_send"), sem("b", g, p), tensor=flip(ten, (q + p) % bits)
            ).start()

    def exchange_f(p):
        for q in range(2):
            span = pl.ds(q * (rows // 2), rows // 2)
            remote(
                send_f.at[p, span], recv_f.at[p, span], sem("f_send"), sem("f", p), tensor=flip(ten, (q + p) % bits)
            ).start()

    def arrived(target, recv):
        remote(target, target, sem("b_send"), recv, tensor=flip(ten, 0)).wait_recv()

    def squares(p):
        return remote(sq_out.at[p], sq_in.at[p], sem("sq", "s", p), sem("sq", "r", p), tensor=flip(ten, p))

    eye = lax.broadcasted_iota(jnp.int32, (rows, rows), 0) == lax.broadcasted_iota(jnp.int32, (rows, rows), 1)

    def to_row(column):
        return jnp.sum(jnp.where(eye, column, 0.0), axis=0, keepdims=True)

    def to_column(row):
        return jnp.sum(jnp.where(eye, row, 0.0), axis=1, keepdims=True)

    def spread(column, count):
        lane = lax.broadcasted_iota(jnp.int32, (column.shape[0], padded - rank), 1)
        result = jnp.zeros(lane.shape, F32)
        for i in range(count):
            piece = column.astype(BF16).astype(F32)
            result = jnp.where(lane == i, piece, result)
            column = column - piece
        return result.astype(BF16)

    for name in ("gain", "sav", "down"):
        loads[name].wait()
    square_s = jnp.zeros((rows, 1), F32)
    total_s = jnp.zeros((rows, rank), F32)
    for cols in columns:
        values = sav[:, cols].astype(F32)
        square_s += jnp.sum(values * values, axis=1, keepdims=True)
        gained = (values * gain[:, cols].astype(F32)).astype(BF16)
        scaled[:, cols] = gained
        total_s += contract_last(gained, down[:, cols])
    square_row = to_row(square_s)
    if bits:
        sq_out[0] = square_row
    for name in ("len", "grad", "up", "fwd"):
        loads[name].wait()

    pl.semaphore_wait(barrier, bits + n_dp - 1 + jnp.where(sec > 0, 1, 0) + jnp.where(sec < n_sec - 1, 1, 0))

    @pl.when(sec > 0)
    def _():
        for copy in (raw_savs, raw_downs, raw_gains):
            copy.start()

    @pl.when(sec < n_sec - 1)
    def _():
        for copy in (raw_ups, raw_fwds):
            copy.start()

    position = lax.broadcasted_iota(jnp.int32, (rows, 1), 0)
    seq_rows = rows // n_seq
    limit = jnp.full((rows, 1), 0, jnp.int32)
    for i in range(n_seq):
        limit = jnp.where(position >= i * seq_rows, i * seq_rows + lens[0, i], limit)
    keep = position < limit
    total_g = jnp.zeros((rows, rank), F32)
    for cols in columns[::-1]:
        held = jnp.where(keep, kept[:, cols].astype(F32), 0.0).astype(BF16)
        kept[:, cols] = held
        total_g += contract_last(held, up[:, cols])
    total_b = jnp.concatenate([total_g, total_s], axis=1)
    acc_b[...] = total_b
    if bits:
        send_b[0] = total_b.astype(BF16)
    if bits:
        for g, (start, size) in enumerate(groups):
            exchange_b(start, size, g, 0)
            if g == 0:
                squares(0).start()

    @pl.when(sec > 0)
    def _():
        raw_keeps.start()

    total = jnp.zeros((rows, rank), F32)
    square_f = jnp.zeros((rows, 1), F32)
    for cols in columns:
        values = fwd[:, cols].astype(F32)
        square_f += jnp.sum(values * values, axis=1, keepdims=True)
        gained = (values * gain[:, cols].astype(F32)).astype(BF16)
        total += contract_last(gained, down[:, cols])

    def begin_f(p):
        send_f[p, :, :rank] = total.astype(BF16)
        send_f[p, :, rank:] = spread(square_f, 3)
        exchange_f(p)

    if bits:
        begin_f(0)
    for p in range(1, bits):
        squares(p - 1).wait_recv()
        square_row += sq_in[p - 1]
        sq_out[p] = square_row
        squares(p).start()
        for g, (start, size) in enumerate(groups):
            span = pl.ds(start, size)
            arrived(recv_b.at[p - 1, span], sem("b", g, p - 1))
            summed = acc_b[span] + recv_b[p - 1, span].astype(F32)
            acc_b[span] = summed
            send_b[p, span] = summed.astype(BF16)
            exchange_b(start, size, g, p)
        arrived(recv_f.at[p - 1], sem("f", p - 1))
        total += recv_f[p - 1, :, :rank].astype(F32)
        square_f += jnp.sum(recv_f[p - 1, :, rank:].astype(F32), axis=1, keepdims=True)
        begin_f(p)

    done_f = [slice(a, min(a + chunk, width - raw_f)) for a in range(0, width - raw_f, chunk)]
    done_b = [slice(a, min(a + chunk, width - raw_b)) for a in range(0, width - raw_b, chunk)]

    def shift(way, start, size, cols):
        source, target = ((out_f, next_in), (out_b, next_gr))[way]
        part_rows, span = pl.ds(start, size), pl.ds(cols.start, cols.stop - cols.start)
        name = ("out_f", "out_b")[way]
        return across(
            1 - 2 * way, source.at[part_rows, span], target.at[part_rows, span], sem(name, "s"), sem(name, "r")
        )

    if bits:
        squares(bits - 1).wait_recv()
        square_row += sq_in[bits - 1]
    scale_s = lax.rsqrt(to_column(square_row) / full_width + EPSILON)
    acts_s, backs_s, tilts = [], [], []

    def give_back(start, size, back_rows, tilt):
        span = slice(start, start + size)
        for cols in done_b:
            normed = jnp.dot(back_rows, down[:, cols], preferred_element_type=F32)
            out_b[span, cols] = (
                kept[span, cols].astype(F32)
                + gain[:, cols].astype(F32) * normed
                - sav[span, cols].astype(F32) * tilt
            ).astype(BF16)
            shift(1, start, size, cols).start()

    for g, (start, size) in enumerate(groups):
        span = slice(start, start + size)
        if bits:
            arrived(recv_b.at[bits - 1, pl.ds(start, size)], sem("b", g, bits - 1))
            summed = acc_b[span] + recv_b[bits - 1, span].astype(F32)
        else:
            summed = acc_b[span]
        own_scale = scale_s[span]
        slope = summed[:, :rank]
        rank_s = summed[:, rank:] * own_scale
        gate = jax.nn.sigmoid(rank_s)
        acts_s.append((rank_s * gate).astype(BF16))
        back = slope * (gate * (1.0 + rank_s * (1.0 - gate)))
        tilts.append(jnp.sum(back.astype(BF16).astype(F32) * rank_s, axis=1, keepdims=True) * (own_scale * own_scale / full_width))
        backs_s.append((back * own_scale).astype(BF16))
        if g == 0 and len(groups) > 1:
            @pl.when(sec > 0)
            def _():
                give_back(start, size, backs_s[0], tilts[0])

    early = 1 if len(groups) > 1 else 0

    @pl.when(sec > 0)
    def _():
        for (start, size), back_rows, tilt in zip(groups, backs_s, tilts):
            back_out[start:start + size, :rank] = back_rows
            back_out[start:start + size, rank:] = spread(tilt, 2)
        backs.start()
        for (start, size), back_rows, tilt in list(zip(groups, backs_s, tilts))[early:]:
            give_back(start, size, back_rows, tilt)

    back_scaled = jnp.concatenate(backs_s, axis=0)
    act_s = jnp.concatenate(acts_s, axis=0)

    if bits:
        arrived(recv_f.at[bits - 1], sem("f", bits - 1))
        total += recv_f[bits - 1, :, :rank].astype(F32)
        square_f += jnp.sum(recv_f[bits - 1, :, rank:].astype(F32), axis=1, keepdims=True)
    rank_f = total * lax.rsqrt(square_f / full_width + EPSILON)
    act_f = (rank_f * jax.nn.sigmoid(rank_f)).astype(BF16)

    @pl.when(sec < n_sec - 1)
    def _():
        act_out[:, :rank] = act_f
        act_out[:, rank:] = jnp.zeros((rows, padded - rank), BF16)
        acts.start()
        for cols in done_f:
            grown = jnp.dot(act_f, up[:, cols], preferred_element_type=F32)
            out_f[:, cols] = (fwd[:, cols].astype(F32) + grown).astype(BF16)
            shift(0, 0, rows, cols).start()

    @pl.when(sec > 0)
    def _():
        raw_ups.wait_recv()
        for k in range(1, n_dp):
            relay(0, k).start()

    @pl.when(sec < n_sec - 1)
    def _():
        raw_downs.wait_recv()
        for k in range(1, n_dp):
            relay(1, k).start()

    def trade(k):
        target = (dp + k) % n_dp
        return remote(
            part.at[:, pl.ds(pl.multiple_of(target * share, share), share)], part_recv.at[k - 1],
            sem("trade", "s", k), sem("trade", "r", k), dp=target,
        )

    for i, (left_side, right_side) in enumerate(((back_scaled, scaled), (act_s, kept))):
        for cols in columns:
            part[i, :, cols] = contract_rows(left_side, right_side[:, cols]).astype(BF16)
    for k in range(1, n_dp):
        trade(k).start()

    @pl.when(sec == 0)
    def _():
        next_in[...] = jnp.zeros_like(next_in)

    @pl.when(sec == n_sec - 1)
    def _():
        next_gr[...] = jnp.zeros_like(next_gr)

    def gather(p):
        held_rows = quarter << p
        block = pl.ds(pl.multiple_of(ten // (1 << p) * held_rows, held_rows), held_rows)
        return remote(pair.at[block], pair.at[block], sem("all", "s", p), sem("all", "r", p), tensor=flip(ten, p))

    @pl.when(sec > 0)
    def _():
        acts.wait_recv()

    @pl.when(sec < n_sec - 1)
    def _():
        backs.wait_recv()

    if bits:
        gather(0).start()

    for k in range(1, n_dp):
        trade(k).wait()
    for i, out in enumerate((grad_down, grad_up)):
        for cols in columns:
            summed = part[i, mine, cols].astype(F32)
            for k in range(1, n_dp):
                summed += part_recv[k - 1, i, :, cols].astype(F32)
            out[:, cols] = (summed * (1.0 / n_dp)).astype(BF16)

    for p in range(bits):
        gather(p).wait()
        if p + 1 < bits:
            gather(p + 1).start()

    @pl.when(sec > 0)
    def _():
        for k in range(1, n_dp):
            relay(0, k).wait()
        raw_fwds.wait_recv()
        for a in range(0, raw_f, chunk):
            b = min(a + chunk, raw_f)
            grown = jnp.dot(pair[:, :rank], raw_up[:, a:b], preferred_element_type=F32)
            next_in[:, width - raw_f + a:width - raw_f + b] = (raw_fwd[:, a:b].astype(F32) + grown).astype(BF16)

    @pl.when(sec < n_sec - 1)
    def _():
        for k in range(1, n_dp):
            relay(1, k).wait()
        raw_gains.wait_recv()
        raw_pairs.wait_recv()
        far_tilt = jnp.sum(pair[:, padded + rank:].astype(F32), axis=1, keepdims=True)
        for a in range(0, raw_b, chunk):
            b = min(a + chunk, raw_b)
            normed = jnp.dot(pair[:, padded:padded + rank], raw_down[:, a:b], preferred_element_type=F32)
            next_gr[:, width - raw_b + a:width - raw_b + b] = (
                raw_pair[1, :, a:b].astype(F32)
                + raw_gain[:, a:b].astype(F32) * normed
                - raw_pair[0, :, a:b].astype(F32) * far_tilt
            ).astype(BF16)

    if bits:
        for p in range(bits):
            squares(p).wait_send()
        remote(send_b, recv_b, sem("b_send"), sem("b", 0, 0), tensor=flip(ten, 0)).wait_send()
        remote(send_f, recv_f, sem("f_send"), sem("f", 0), tensor=flip(ten, 0)).wait_send()

    whole_f = across(1, fwd, out_f, sem("out_f", "s"), sem("out_f", "r"))
    whole_b = across(-1, kept, out_b, sem("out_b", "s"), sem("out_b", "r"))

    @pl.when(sec < n_sec - 1)
    def _():
        for copy in (raw_ups, acts, whole_f):
            copy.wait_send()

    @pl.when(sec > 0)
    def _():
        for copy in (raw_savs, raw_downs, raw_gains, backs, whole_b):
            copy.wait_send()

    @pl.when(sec < n_sec - 1)
    def _():
        shift(1, 0, rows, slice(0, width - raw_b)).wait_recv()

    @pl.when(sec > 0)
    def _():
        shift(0, 0, rows, slice(0, width - raw_f)).wait_recv()


def place(*refs):
    count = len(refs) // 2
    sems = refs[-1]
    copies = [pltpu.make_async_copy(refs[i], refs[count + i], sems.at[i]) for i in range(count)]
    for copy in copies:
        copy.start()
    for copy in copies:
        copy.wait()


def solution(mesh):
    n_sec, n_ten, n_dp = (mesh.shape[name] for name in ("section", "tensor", "dp"))

    def shards(forward_rows, saved_rows, output_grad, lengths, norm_gain, down_map, up_map):
        rows, width = forward_rows.shape[2:]
        rank = down_map.shape[1]
        n_seq = lengths.shape[2]
        share = rank // n_dp
        bits = n_ten.bit_length() - 1
        chunk = min(width, 4 * LANES)
        raw_f = int(width * RAW_FORWARD) // LANES * LANES
        raw_b = int(width * RAW_BACK) // LANES * LANES
        steps = max(bits, 1)
        padded = (rank + 3 + LANES - 1) // LANES * LANES
        vmem = pl.BlockSpec(memory_space=pltpu.VMEM)
        anywhere = pl.BlockSpec(memory_space=pl.ANY)
        flops = 7 * 2 * rows * rank * width
        dma = pltpu.SemaphoreType.DMA
        shapes = ((rows, width),) * 2 + ((share, width),) * 2
        results = pl.pallas_call(
            functools.partial(tick, (n_sec, n_ten, n_dp, chunk)),
            out_shape=tuple(pltpu.VMEM(shape, BF16) for shape in shapes),
            in_specs=[anywhere] * 7,
            out_specs=(vmem,) * 4,
            scratch_shapes=[
                pltpu.SMEM((1, n_seq), jnp.int32),
                pltpu.VMEM((1, width), BF16),
                pltpu.VMEM((rows, width), BF16),
                pltpu.VMEM((rows, width), BF16),
                pltpu.VMEM((rows, width), BF16),
                pltpu.VMEM((rank, width), BF16),
                pltpu.VMEM((rank, width), BF16),
                pltpu.VMEM((rows, width), BF16),
                pltpu.VMEM((rows, padded), F32),
                pltpu.VMEM((rows, 2 * rank), F32),
                pltpu.VMEM((steps, rows, padded), BF16),
                pltpu.VMEM((steps, rows, padded), BF16),
                pltpu.VMEM((steps, rows, 2 * rank), BF16),
                pltpu.VMEM((steps, rows, 2 * rank), BF16),
                pltpu.VMEM((rows, width), BF16),
                pltpu.VMEM((rows, width), BF16),
                pltpu.VMEM((2, rank, width), BF16),
                pltpu.VMEM((max(n_dp - 1, 1), 2, share, width), BF16),
                pltpu.VMEM((rows, padded), BF16),
                pltpu.VMEM((rows, padded), BF16),
                pltpu.VMEM((rows, 2 * padded), BF16),
                pltpu.VMEM((steps, 1, rows), F32),
                pltpu.VMEM((steps, 1, rows), F32),
                pltpu.VMEM((rows, raw_f), BF16),
                pltpu.VMEM((rank, raw_f), BF16),
                pltpu.VMEM((2, rows, raw_b), BF16),
                pltpu.VMEM((rank, raw_b), BF16),
                pltpu.VMEM((1, raw_b), BF16),
                dma((len(semaphores(len(row_groups(rows)), bits, n_dp)),)),
            ],
            compiler_params=pltpu.CompilerParams(collective_id=0, has_side_effects=True),
            cost_estimate=pl.CostEstimate(
                flops=flops, bytes_accessed=16 * rows * width, transcendentals=4 * rows * rank
            ),
            name="tick",
        )(
            forward_rows[0, 0], saved_rows[0, 0], output_grad[0, 0], lengths[0], norm_gain, down_map[0], up_map[0]
        )
        next_inputs, next_grads, grad_down, grad_up = pl.pallas_call(
            place,
            out_shape=tuple(jax.ShapeDtypeStruct(shape, BF16) for shape in shapes),
            in_specs=[vmem] * 4,
            out_specs=(anywhere,) * 4,
            scratch_shapes=[dma((4,))],
            name="place",
        )(*[pltpu.with_memory_space_constraint(x, pltpu.VMEM) for x in results])
        return next_inputs[None, None], next_grads[None, None], grad_down[None], grad_up[None]

    row_spec = P("section", "dp", None, "tensor")
    map_spec = P("section", None, "tensor")
    part_spec = P("section", "dp", "tensor")
    return jax.shard_map(
        shards,
        mesh=mesh,
        in_specs=(row_spec, row_spec, row_spec, P("section", "dp"), P("section", "tensor"), map_spec, map_spec),
        out_specs=(row_spec, row_spec, part_spec, part_spec),
        check_vma=False,
    )
```

```python
import functools

import jax
import jax.numpy as jnp
from jax import lax
from jax.experimental import pallas as pl
from jax.experimental.pallas import tpu as pltpu
from jax.sharding import PartitionSpec as P

EPSILON = 1e-05
LANES = 128
RAW_FORWARD = 0.375
RAW_BACK = 0.125
F32 = jnp.float32
BF16 = jnp.bfloat16


def contract_last(left_side, right_side):
    return lax.dot_general(
        left_side, right_side, (((1,), (1,)), ((), ())), preferred_element_type=F32
    )


def contract_rows(left_side, right_side):
    return lax.dot_general(
        left_side, right_side, (((0,), (0,)), ((), ())), preferred_element_type=F32
    )


def flip(index, bit):
    step = 1 << bit
    return index + step * (1 - 2 * ((index // step) % 2))


def peer(index, k, bits):
    for bit in range(bits):
        if k >> bit & 1:
            index = flip(index, bit)
    return index


def row_groups(rows):
    sizes = (rows // 6, rows // 3, rows // 2) if rows % 192 == 0 else (rows,)
    starts = [sum(sizes[:i]) for i in range(len(sizes))]
    return list(zip(starts, sizes))


def semaphores(n_group, bits, n_dp):
    names = ["len", "gain", "fwd", "sav_tail", "sav", "down", "kept_up"]
    names += [(side, kind) for side in ("sq", "first") for kind in "sr"]
    names += [("b", g, p) for g in range(1, n_group) for p in range(bits)] + ["b_send"]
    names += [("f", p) for p in range(bits)] + ["f_send"]
    names += [(side, kind) for side in ("out_f", "out_b") for kind in "sr"]
    names += [(side, kind) for side in ("raw_up", "raw_down", "act", "back") for kind in "sr"]
    names += ["raw_fwd_r", "raw_sav_s", "raw_pair_r"]
    names += [("all", kind, p) for kind in "sr" for p in range(bits)]
    names += [("trade", kind, k) for kind in "sr" for k in range(1, n_dp)]
    names += [("relay", way, kind, k) for way in range(2) for kind in "sr" for k in range(1, n_dp)]
    return {name: i for i, name in enumerate(names)}


def tick(sizes, fwd_hbm, sav_hbm, grad_hbm, len_hbm, gain_hbm, down_hbm, up_hbm,
         next_in, next_gr, grad_down, grad_up,
         lens, gain, fwd, sav_down, kept_up, gained,
         acc_b, send_f, recv_f, send_b, recv_b, first_b, out_f, out_b,
         part, part_recv, act_out, back_out, pair, sq_out, sq_in,
         raw_fwd, raw_up, raw_pair, raw_down, sems, far_sem):
    n_sec, n_ten, n_dp, chunk = sizes
    rows, width = fwd.shape
    rank = down_hbm.shape[0]
    sav, down = sav_down.at[pl.ds(0, rows)], sav_down.at[pl.ds(rows, rank)]
    kept, up = kept_up.at[pl.ds(0, rows)], kept_up.at[pl.ds(rows, rank)]
    padded = act_out.shape[1]
    full_width = width * n_ten
    n_seq = lens.shape[1]
    bits = n_ten.bit_length() - 1
    share = rank // n_dp
    quarter = rows // n_ten
    groups = row_groups(rows)
    columns = [slice(c, c + chunk) for c in range(0, width, chunk)]
    index = semaphores(len(groups), bits, n_dp)
    sec, ten, dp = lax.axis_index("section"), lax.axis_index("tensor"), lax.axis_index("dp")

    def sem(*name):
        return sems.at[index[name if len(name) > 1 else name[0]]]

    @pl.when(sec == 0)
    def _():
        pair[:, :padded] = jnp.zeros((rows, padded), BF16)

    @pl.when(sec == n_sec - 1)
    def _():
        pair[:, padded:] = jnp.zeros((rows, padded), BF16)

    barrier = pltpu.get_barrier_semaphore()
    relayed = bits == 2
    near = [1 << bit for bit in range(bits)] if relayed else range(1, n_ten)
    for k in near:
        pl.semaphore_signal(barrier, inc=1, device_id={"tensor": peer(ten, k, bits)})
    for k in range(1, n_dp):
        pl.semaphore_signal(barrier, inc=1, device_id={"dp": (dp + k) % n_dp})

    @pl.when(sec > 0)
    def _():
        pl.semaphore_signal(barrier, inc=1, device_id={"section": sec - 1})

    @pl.when(sec < n_sec - 1)
    def _():
        pl.semaphore_signal(barrier, inc=1, device_id={"section": sec + 1})

    raw_f, raw_b = raw_fwd.shape[1], raw_pair.shape[2]
    mine = pl.ds(pl.multiple_of(dp * share, share), share)
    own = pl.ds(pl.multiple_of(ten * quarter, quarter), quarter)
    tail_f, tail_b = pl.ds(width - raw_f, raw_f), pl.ds(width - raw_b, raw_b)
    loads = {
        name: pltpu.make_async_copy(source, target, sem(name))
        for name, source, target in (
            ("gain", gain_hbm, gain), ("len", len_hbm, lens), ("fwd", fwd_hbm, fwd),
            ("sav_tail", sav_hbm.at[:, tail_b], sav.at[:, tail_b]),
            ("sav", sav_hbm.at[:, pl.ds(0, width - raw_b)], sav.at[:, pl.ds(0, width - raw_b)]),
            ("down", down_hbm, down),
        )
    }
    loads["sav_tail"].start()
    loads["gain"].start()
    loads["sav"].start()
    loads["down"].start()
    for name, both, sources in (("kept_up", kept_up, (grad_hbm, up_hbm)),):
        loads[name] = pltpu.make_async_copy(both, both, sem(name))
        for source, first in zip(sources, (0, rows)):
            pltpu.make_async_copy(source, both.at[pl.ds(first, source.shape[0])], sem(name)).start()
    loads["len"].start()
    loads["fwd"].start()


    def remote(source, target, send, recv, **place):
        return pltpu.make_async_remote_copy(
            src_ref=source, dst_ref=target, send_sem=send, recv_sem=recv, device_id=place
        )

    def across(step, source, target, send, recv):
        return remote(source, target, send, recv, section=sec + step)

    raw_ups = across(1, up.at[mine, tail_f], raw_up.at[mine], sem("raw_up", "s"), sem("raw_up", "r"))
    raw_fwds = across(1, fwd.at[:, tail_f], raw_fwd, sem("out_f", "s"), sem("raw_fwd_r"))
    acts = across(1, act_out.at[own], pair.at[own, pl.ds(0, padded)], sem("act", "s"), sem("act", "r"))
    raw_downs = across(-1, gained.at[mine, tail_b], raw_down.at[mine], sem("raw_down", "s"), sem("raw_down", "r"))
    raw_savs = across(-1, sav.at[:, tail_b], raw_pair.at[0], sem("raw_sav_s"), sem("raw_pair_r"))
    raw_keeps = across(-1, kept.at[:, tail_b], raw_pair.at[1], sem("out_b", "s"), sem("raw_pair_r"))
    raw_pairs = across(-1, raw_pair, raw_pair, sem("raw_sav_s"), sem("raw_pair_r"))
    backs = across(-1, back_out.at[own], pair.at[own, pl.ds(padded, padded)], sem("back", "s"), sem("back", "r"))

    def relay(way, k):
        ref = (raw_up, raw_down)[way].at[mine]
        return remote(ref, ref, sem("relay", way, "s", k), sem("relay", way, "r", k), dp=(dp + k) % n_dp)

    first_rows = groups[0][1]

    def exchange_first():
        for k in range(n_ten - 1, 0, -1):
            place = {"tensor": peer(ten, k, bits)}
            remote(
                send_b.at[0, pl.ds(0, first_rows)], first_b.at[k - 1], sem("first", "s"), sem("first", "r"), **place
            ).start()
            remote(sq_out, sq_in.at[k - 1], sem("sq", "s"), sem("sq", "r"), **place).start()

    def exchange_b(start, size, g, p):
        for q in range(2):
            span = pl.ds(start + q * (size // 2), size // 2)
            remote(
                send_b.at[p, span], recv_b.at[p, span], sem("b_send"), sem("b", g, p), tensor=flip(ten, (q + p) % bits)
            ).start()

    def exchange_f(p):
        for q in range(2):
            span = pl.ds(q * (rows // 2), rows // 2)
            remote(
                send_f.at[p, span], recv_f.at[p, span], sem("f_send"), sem("f", p), tensor=flip(ten, (q + p) % bits)
            ).start()

    def arrived(target, recv):
        remote(target, target, sem("f_send"), recv, tensor=flip(ten, 0)).wait_recv()

    eye = lax.broadcasted_iota(jnp.int32, (rows, rows), 0) == lax.broadcasted_iota(jnp.int32, (rows, rows), 1)

    def to_row(column):
        return jnp.sum(jnp.where(eye, column, 0.0), axis=0, keepdims=True)

    def to_column(row):
        return jnp.sum(jnp.where(eye, row, 0.0), axis=1, keepdims=True)

    def spread(column, count):
        lane = lax.broadcasted_iota(jnp.int32, (column.shape[0], padded - rank), 1)
        result = jnp.zeros(lane.shape, F32)
        for i in range(count):
            piece = column.astype(BF16).astype(F32)
            result = jnp.where(lane == i, piece, result)
            column = column - piece
        return result.astype(BF16)

    loads["sav_tail"].wait()

    pl.semaphore_wait(barrier, len(near) + n_dp - 1 + jnp.where(sec > 0, 1, 0) + jnp.where(sec < n_sec - 1, 1, 0))
    if relayed:
        pl.semaphore_signal(far_sem, inc=1, device_id={"tensor": flip(ten, 0)})

    @pl.when(sec > 0)
    def _():
        raw_savs.start()

    for name in ("gain", "sav", "down"):
        loads[name].wait()
    square_s = jnp.zeros((rows, 1), F32)
    total_s = jnp.zeros((rows, rank), F32)
    for cols in columns:
        values = sav[:, cols].astype(F32)
        square_s += jnp.sum(values * values, axis=1, keepdims=True)
        scaled = down[:, cols] * gain[:, cols]
        gained[:, cols] = scaled
        total_s += contract_last(sav[:, cols], scaled)
    square_row = to_row(square_s)
    if bits:
        sq_out[...] = square_row

    @pl.when(sec > 0)
    def _():
        raw_downs.start()

    loads["len"].wait()
    loads["kept_up"].wait()

    @pl.when(sec < n_sec - 1)
    def _():
        raw_ups.start()

    position = lax.broadcasted_iota(jnp.int32, (rows, 1), 0)
    seq_rows = rows // n_seq
    limit = jnp.full((rows, 1), 0, jnp.int32)
    for i in range(n_seq):
        limit = jnp.where(position >= i * seq_rows, i * seq_rows + lens[0, i], limit)
    keep = position < limit
    total_g = jnp.zeros((rows, rank), F32)
    for cols in columns:
        total_g += contract_last(kept[:, cols], up[:, cols])
    total_b = jnp.concatenate([jnp.where(keep, total_g, 0.0), total_s], axis=1)
    acc_b[...] = total_b
    if bits:
        send_b[0] = total_b.astype(BF16)
        if relayed:
            pl.semaphore_wait(far_sem, 1)
        exchange_first()
        for g, (start, size) in list(enumerate(groups))[1:]:
            exchange_b(start, size, g, 0)

    loads["fwd"].wait()

    @pl.when(sec < n_sec - 1)
    def _():
        raw_fwds.start()

    for cols in columns[::-1]:
        kept[:, cols] = jnp.where(keep, kept[:, cols].astype(F32), 0.0).astype(BF16)

    @pl.when(sec > 0)
    def _():
        raw_keeps.start()

    total = jnp.zeros((rows, rank), F32)
    square_f = jnp.zeros((rows, 1), F32)
    for cols in columns:
        values = fwd[:, cols].astype(F32)
        square_f += jnp.sum(values * values, axis=1, keepdims=True)
        total += contract_last(fwd[:, cols], gained[:, cols])

    def begin_f(p, total, square_f):
        send_f[p, :, :rank] = total.astype(BF16)
        send_f[p, :, rank:] = spread(square_f, 3)
        exchange_f(p)

    if bits:
        begin_f(0, total, square_f)
    def step_b(p, chosen):
        for g, (start, size) in chosen:
            span = pl.ds(start, size)
            arrived(recv_b.at[p - 1, span], sem("b", g, p - 1))
            summed = acc_b[span] + recv_b[p - 1, span].astype(F32)
            acc_b[span] = summed
            send_b[p, span] = summed.astype(BF16)
            exchange_b(start, size, g, p)

    later = list(enumerate(groups))[1:]
    if bits > 1:
        step_b(1, later[:1])

    done_f = [slice(a, min(a + chunk, width - raw_f)) for a in range(0, width - raw_f, chunk)]
    done_b = [slice(a, min(a + chunk, width - raw_b)) for a in range(0, width - raw_b, chunk)]

    def shift(way, start, size, cols):
        source, target = ((out_f, next_in), (out_b, next_gr))[way]
        part_rows, span = pl.ds(start, size), pl.ds(cols.start, cols.stop - cols.start)
        name = ("out_f", "out_b")[way]
        return across(
            1 - 2 * way, source.at[part_rows, span], target.at[part_rows, span], sem(name, "s"), sem(name, "r")
        )

    if bits:
        arrived(sq_in, sem("sq", "r"))
        for k in range(1, n_ten):
            square_row += sq_in[k - 1]
    scale_s = lax.rsqrt(to_column(square_row) / full_width + EPSILON)
    acts_s, backs_s, tilts = [], [], []

    def give_back(start, size, back_rows, tilt, first):
        span = slice(start, start + size)
        for cols in done_b:
            normed = jnp.dot(back_rows, gained[:, cols], preferred_element_type=F32)
            out_b[span, cols] = (
                kept[span, cols].astype(F32)
                + normed
                - sav[span, cols].astype(F32) * tilt
            ).astype(BF16)
            if first or cols in done_b[:1]:
                shift(1, start, size, cols).start()

    def send_late():
        start, size = groups[-1]
        for cols in done_b[1:]:
            shift(1, start, size, cols).start()

    for g, (start, size) in enumerate(groups):
        span = slice(start, start + size)
        if bits and g == 0:
            arrived(first_b, sem("first", "r"))
            summed = acc_b[span]
            for k in range(1, n_ten):
                summed += first_b[k - 1].astype(F32)
        elif bits:
            arrived(recv_b.at[bits - 1, pl.ds(start, size)], sem("b", g, bits - 1))
            summed = acc_b[span] + recv_b[bits - 1, span].astype(F32)
        else:
            summed = acc_b[span]
        own_scale = scale_s[span]
        slope = summed[:, :rank]
        rank_s = summed[:, rank:] * own_scale
        gate = jax.nn.sigmoid(rank_s)
        acts_s.append((rank_s * gate).astype(BF16))
        back = slope * (gate * (1.0 + rank_s * (1.0 - gate)))
        tilts.append(jnp.sum(back.astype(BF16).astype(F32) * rank_s, axis=1, keepdims=True) * (own_scale * own_scale / full_width))
        backs_s.append((back * own_scale).astype(BF16))
        if g == 0 and len(groups) > 1:
            @pl.when(sec > 0)
            def _():
                give_back(start, size, backs_s[0], tilts[0], True)
        if 0 < g < len(groups) - 1:
            @pl.when(jnp.logical_and(sec > 0, dp % 2 == 1))
            def _():
                give_back(start, size, backs_s[g], tilts[g], True)
        if g == 0:
            for p in range(1, bits):
                step_b(p, later[1:] if p == 1 else later)
            for p in range(1, bits):
                arrived(recv_f.at[p - 1], sem("f", p - 1))
                total += recv_f[p - 1, :, :rank].astype(F32)
                square_f += jnp.sum(recv_f[p - 1, :, rank:].astype(F32), axis=1, keepdims=True)
                begin_f(p, total, square_f)

    early = 1 if len(groups) > 1 else 0

    @pl.when(sec > 0)
    def _():
        for (start, size), back_rows, tilt in zip(groups, backs_s, tilts):
            back_out[start:start + size, :rank] = back_rows
            back_out[start:start + size, rank:] = spread(tilt, 2)
        backs.start()
        for g in range(early, len(groups) - 1):
            @pl.when(dp % 2 == 0)
            def _():
                give_back(*groups[g], backs_s[g], tilts[g], True)
        give_back(*groups[-1], backs_s[-1], tilts[-1], False)
        pl.when(dp % 2 == 0)(send_late)

    back_scaled = jnp.concatenate(backs_s, axis=0)
    act_s = jnp.concatenate(acts_s, axis=0)

    if bits:
        arrived(recv_f.at[bits - 1], sem("f", bits - 1))
        total += recv_f[bits - 1, :, :rank].astype(F32)
        square_f += jnp.sum(recv_f[bits - 1, :, rank:].astype(F32), axis=1, keepdims=True)
    rank_f = total * lax.rsqrt(square_f / full_width + EPSILON)
    act_f = (rank_f * jax.nn.sigmoid(rank_f)).astype(BF16)

    @pl.when(sec < n_sec - 1)
    def _():
        act_out[:, :rank] = act_f
        act_out[:, rank:] = jnp.zeros((rows, padded - rank), BF16)
        acts.start()
        for cols in done_f:
            grown = jnp.dot(act_f, up[:, cols], preferred_element_type=F32)
            out_f[:, cols] = (fwd[:, cols].astype(F32) + grown).astype(BF16)
            shift(0, 0, rows, cols).start()

    @pl.when(sec > 0)
    def _():
        raw_ups.wait_recv()
        for k in range(1, n_dp):
            relay(0, k).start()

    @pl.when(sec < n_sec - 1)
    def _():
        raw_downs.wait_recv()
        for k in range(1, n_dp):
            relay(1, k).start()

    def trade(k):
        target = (dp + k) % n_dp
        return remote(
            part.at[:, pl.ds(pl.multiple_of(target * share, share), share)], part_recv.at[k - 1],
            sem("trade", "s", k), sem("trade", "r", k), dp=target,
        )

    for cols in columns:
        part[0, :, cols] = (contract_rows(back_scaled, sav[:, cols]) * gain[:, cols].astype(F32)).astype(BF16)
        part[1, :, cols] = contract_rows(act_s, kept[:, cols]).astype(BF16)
    for k in range(1, n_dp):
        trade(k).start()

    @pl.when(sec == 0)
    def _():
        next_in[...] = jnp.zeros_like(next_in)

    @pl.when(sec == n_sec - 1)
    def _():
        next_gr[...] = jnp.zeros_like(next_gr)

    def gather(p):
        held_rows = quarter << p
        block = pl.ds(pl.multiple_of(ten // (1 << p) * held_rows, held_rows), held_rows)
        return remote(pair.at[block], pair.at[block], sem("all", "s", p), sem("all", "r", p), tensor=flip(ten, p))

    @pl.when(sec > 0)
    def _():
        acts.wait_recv()

    @pl.when(sec < n_sec - 1)
    def _():
        backs.wait_recv()

    if bits:
        gather(0).start()

    for k in range(1, n_dp):
        trade(k).wait()
    for i, out in enumerate((grad_down, grad_up)):
        for cols in columns:
            summed = part[i, mine, cols].astype(F32)
            for k in range(1, n_dp):
                summed += part_recv[k - 1, i, :, cols].astype(F32)
            out[:, cols] = (summed * (1.0 / n_dp)).astype(BF16)

    for p in range(bits):
        gather(p).wait()
        if p + 1 < bits:
            gather(p + 1).start()
        if p == 0:
            pl.when(jnp.logical_and(sec > 0, dp % 2 == 1))(send_late)

    @pl.when(sec > 0)
    def _():
        for k in range(1, n_dp):
            relay(0, k).wait()
        raw_fwds.wait_recv()
        for a in range(0, raw_f, chunk):
            b = min(a + chunk, raw_f)
            grown = jnp.dot(pair[:, :rank], raw_up[:, a:b], preferred_element_type=F32)
            next_in[:, width - raw_f + a:width - raw_f + b] = (raw_fwd[:, a:b].astype(F32) + grown).astype(BF16)

    @pl.when(sec < n_sec - 1)
    def _():
        for k in range(1, n_dp):
            relay(1, k).wait()
        raw_pairs.wait_recv()
        far_tilt = jnp.sum(pair[:, padded + rank:].astype(F32), axis=1, keepdims=True)
        for a in range(0, raw_b, chunk):
            b = min(a + chunk, raw_b)
            normed = jnp.dot(pair[:, padded:padded + rank], raw_down[:, a:b], preferred_element_type=F32)
            next_gr[:, width - raw_b + a:width - raw_b + b] = (
                raw_pair[1, :, a:b].astype(F32)
                + normed
                - raw_pair[0, :, a:b].astype(F32) * far_tilt
            ).astype(BF16)

    if bits:
        remote(sq_in, sq_in, sem("sq", "s"), sem("sq", "r"), tensor=flip(ten, 0)).wait_send()
        remote(first_b, first_b, sem("first", "s"), sem("first", "r"), tensor=flip(ten, 0)).wait_send()
        if len(groups) > 1:
            rest = send_b.at[:, pl.ds(first_rows, rows - first_rows)]
            remote(rest, rest, sem("b_send"), sem("first", "r"), tensor=flip(ten, 0)).wait_send()
        remote(send_f, recv_f, sem("f_send"), sem("f", 0), tensor=flip(ten, 0)).wait_send()

    whole_f = across(1, fwd, out_f, sem("out_f", "s"), sem("out_f", "r"))
    whole_b = across(-1, kept, out_b, sem("out_b", "s"), sem("out_b", "r"))

    @pl.when(sec < n_sec - 1)
    def _():
        for copy in (raw_ups, acts, whole_f):
            copy.wait_send()

    @pl.when(sec > 0)
    def _():
        for copy in (raw_savs, raw_downs, backs, whole_b):
            copy.wait_send()

    @pl.when(sec < n_sec - 1)
    def _():
        shift(1, 0, rows, slice(0, width - raw_b)).wait_recv()

    @pl.when(sec > 0)
    def _():
        shift(0, 0, rows, slice(0, width - raw_f)).wait_recv()


def place(*refs):
    count = len(refs) // 2
    sems = refs[-1]
    copies = [pltpu.make_async_copy(refs[i], refs[count + i], sems.at[i]) for i in range(count)]
    for copy in copies:
        copy.start()
    for copy in copies:
        copy.wait()


def solution(mesh):
    n_sec, n_ten, n_dp = (mesh.shape[name] for name in ("section", "tensor", "dp"))

    def shards(forward_rows, saved_rows, output_grad, lengths, norm_gain, down_map, up_map):
        rows, width = forward_rows.shape[2:]
        rank = down_map.shape[1]
        n_seq = lengths.shape[2]
        share = rank // n_dp
        bits = n_ten.bit_length() - 1
        chunk = min(width, 4 * LANES)
        raw_f = int(width * RAW_FORWARD) // LANES * LANES
        raw_b = int(width * RAW_BACK) // LANES * LANES
        steps = max(bits, 1)
        padded = (rank + 3 + LANES - 1) // LANES * LANES
        vmem = pl.BlockSpec(memory_space=pltpu.VMEM)
        anywhere = pl.BlockSpec(memory_space=pl.ANY)
        flops = 7 * 2 * rows * rank * width
        dma = pltpu.SemaphoreType.DMA
        shapes = ((rows, width),) * 2 + ((share, width),) * 2
        results = pl.pallas_call(
            functools.partial(tick, (n_sec, n_ten, n_dp, chunk)),
            out_shape=tuple(pltpu.VMEM(shape, BF16) for shape in shapes),
            in_specs=[anywhere] * 7,
            out_specs=(vmem,) * 4,
            scratch_shapes=[
                pltpu.SMEM((1, n_seq), jnp.int32),
                pltpu.VMEM((1, width), BF16),
                pltpu.VMEM((rows, width), BF16),
                pltpu.VMEM((rows + rank, width), BF16),
                pltpu.VMEM((rows + rank, width), BF16),
                pltpu.VMEM((rows, width), BF16),
                pltpu.VMEM((rows, 2 * rank), F32),
                pltpu.VMEM((steps, rows, padded), BF16),
                pltpu.VMEM((steps, rows, padded), BF16),
                pltpu.VMEM((steps, rows, 2 * rank), BF16),
                pltpu.VMEM((steps, rows, 2 * rank), BF16),
                pltpu.VMEM((max(n_ten - 1, 1), row_groups(rows)[0][1], 2 * rank), BF16),
                pltpu.VMEM((rows, width), BF16),
                pltpu.VMEM((rows, width), BF16),
                pltpu.VMEM((2, rank, width), BF16),
                pltpu.VMEM((max(n_dp - 1, 1), 2, share, width), BF16),
                pltpu.VMEM((rows, padded), BF16),
                pltpu.VMEM((rows, padded), BF16),
                pltpu.VMEM((rows, 2 * padded), BF16),
                pltpu.VMEM((1, rows), F32),
                pltpu.VMEM((max(n_ten - 1, 1), 1, rows), F32),
                pltpu.VMEM((rows, raw_f), BF16),
                pltpu.VMEM((rank, raw_f), BF16),
                pltpu.VMEM((2, rows, raw_b), BF16),
                pltpu.VMEM((rank, raw_b), BF16),
                dma((len(semaphores(len(row_groups(rows)), bits, n_dp)),)),
                pltpu.SemaphoreType.REGULAR,
            ],
            compiler_params=pltpu.CompilerParams(collective_id=0, has_side_effects=True),
            cost_estimate=pl.CostEstimate(
                flops=flops, bytes_accessed=16 * rows * width, transcendentals=4 * rows * rank
            ),
            name="tick",
        )(
            forward_rows[0, 0], saved_rows[0, 0], output_grad[0, 0], lengths[0], norm_gain, down_map[0], up_map[0]
        )
        next_inputs, next_grads, grad_down, grad_up = pl.pallas_call(
            place,
            out_shape=tuple(jax.ShapeDtypeStruct(shape, BF16) for shape in shapes),
            in_specs=[vmem] * 4,
            out_specs=(anywhere,) * 4,
            scratch_shapes=[dma((4,))],
            name="place",
        )(*[pltpu.with_memory_space_constraint(x, pltpu.VMEM) for x in results])
        return next_inputs[None, None], next_grads[None, None], grad_down[None], grad_up[None]

    row_spec = P("section", "dp", None, "tensor")
    map_spec = P("section", None, "tensor")
    part_spec = P("section", "dp", "tensor")
    return jax.shard_map(
        shards,
        mesh=mesh,
        in_specs=(row_spec, row_spec, row_spec, P("section", "dp"), P("section", "tensor"), map_spec, map_spec),
        out_specs=(row_spec, row_spec, part_spec, part_spec),
        check_vma=False,
    )
```

```python
import functools

import jax
import jax.numpy as jnp
from jax import lax
from jax.experimental import pallas as pl
from jax.experimental.pallas import tpu as pltpu
from jax.sharding import PartitionSpec as P

EPSILON = 1e-05
LANES = 128
RAW_FORWARD = 0.375
RAW_BACK = 0.125
F32 = jnp.float32
BF16 = jnp.bfloat16


def contract_last(left_side, right_side):
    return lax.dot_general(
        left_side, right_side, (((1,), (1,)), ((), ())), preferred_element_type=F32
    )


def contract_rows(left_side, right_side):
    return lax.dot_general(
        left_side, right_side, (((0,), (0,)), ((), ())), preferred_element_type=F32
    )


def flip(index, bit):
    step = 1 << bit
    return index + step * (1 - 2 * ((index // step) % 2))


def peer(index, k, bits):
    for bit in range(bits):
        if k >> bit & 1:
            index = flip(index, bit)
    return index


def row_groups(rows):
    sizes = (rows // 6, rows // 3, rows // 2) if rows % 192 == 0 else (rows,)
    starts = [sum(sizes[:i]) for i in range(len(sizes))]
    return list(zip(starts, sizes))


def semaphores(n_group, bits, n_dp):
    names = ["len", "gain", "fwd", "sav_tail", "sav", "down", "kept_up"]
    n_load = len(names)
    names += [(side, kind) for side in ("sq", "first") for kind in "sr"]
    names += [("b", g, p) for g in range(1, n_group) for p in range(bits)] + ["b_send"]
    names += [("f", p) for p in range(bits)] + ["f_send"]
    names += [(side, kind) for side in ("out_f", "out_b") for kind in "sr"]
    names += [(side, kind) for side in ("raw_up", "raw_down") for kind in "sr"] + [("act", "r"), ("back", "r")]
    names += ["raw_fwd_r", "raw_sav_s", "raw_pair_r", ("relief", "s"), ("relief", "r")]
    names += [("all", "r", p) for p in range(bits)] + [("trade", "r", k) for k in range(1, n_dp)]
    names += [("relay", way, "r", k) for way in range(2) for k in range(1, n_dp)]
    sends = [("act", "s"), ("back", "s")] + [("all", "s", p) for p in range(bits)]
    sends += [("trade", "s", k) for k in range(1, n_dp)]
    sends += [("relay", way, "s", k) for way in range(2) for k in range(1, n_dp)]
    names += sends[n_load:]
    index = {name: i for i, name in enumerate(names)}
    return index | {name: i for i, name in enumerate(sends[:n_load])}


def tick(sizes, fwd_hbm, sav_hbm, grad_hbm, len_hbm, gain_hbm, down_hbm, up_hbm,
         next_in, next_gr, grad_down, grad_up,
         lens, gain, fwd, sav_down, kept_up, gained,
         acc_b, send_f, recv_f, send_b, recv_b, first_b, out_f, out_b,
         part, part_recv, act_out, back_out, pair, sq_out, sq_in,
         raw_fwd, raw_up, raw_pair, raw_down, relief, sems, far_sem):
    n_sec, n_ten, n_dp, chunk = sizes
    rows, width = fwd.shape
    rank = down_hbm.shape[0]
    sav, down = sav_down.at[pl.ds(0, rows)], sav_down.at[pl.ds(rows, rank)]
    kept, up = kept_up.at[pl.ds(0, rows)], kept_up.at[pl.ds(rows, rank)]
    padded = act_out.shape[1]
    full_width = width * n_ten
    n_seq = lens.shape[1]
    bits = n_ten.bit_length() - 1
    share = rank // n_dp
    quarter = rows // n_ten
    groups = row_groups(rows)
    columns = [slice(c, c + chunk) for c in range(0, width, chunk)]
    index = semaphores(len(groups), bits, n_dp)
    sec, ten, dp = lax.axis_index("section"), lax.axis_index("tensor"), lax.axis_index("dp")

    def sem(*name):
        return sems.at[index[name if len(name) > 1 else name[0]]]

    @pl.when(sec == 0)
    def _():
        pair[:, :padded] = jnp.zeros((rows, padded), BF16)

    @pl.when(sec == n_sec - 1)
    def _():
        pair[:, padded:] = jnp.zeros((rows, padded), BF16)

    barrier = pltpu.get_barrier_semaphore()
    relayed = bits == 2
    near = [1 << bit for bit in range(bits)] if relayed else range(1, n_ten)
    for k in near:
        pl.semaphore_signal(barrier, inc=1, device_id={"tensor": peer(ten, k, bits)})
    for k in range(1, n_dp):
        pl.semaphore_signal(barrier, inc=1, device_id={"dp": (dp + k) % n_dp})

    @pl.when(sec > 0)
    def _():
        pl.semaphore_signal(barrier, inc=1, device_id={"section": sec - 1})

    @pl.when(sec < n_sec - 1)
    def _():
        pl.semaphore_signal(barrier, inc=1, device_id={"section": sec + 1})

    raw_f, raw_b = raw_fwd.shape[1], raw_pair.shape[2]
    mine = pl.ds(pl.multiple_of(dp * share, share), share)
    own = pl.ds(pl.multiple_of(ten * quarter, quarter), quarter)
    tail_f, tail_b = pl.ds(width - raw_f, raw_f), pl.ds(width - raw_b, raw_b)
    loads = {
        name: pltpu.make_async_copy(source, target, sem(name))
        for name, source, target in (
            ("gain", gain_hbm, gain), ("len", len_hbm, lens), ("fwd", fwd_hbm, fwd),
            ("sav_tail", sav_hbm.at[:, tail_b], sav.at[:, tail_b]),
            ("sav", sav_hbm.at[:, pl.ds(0, width - raw_b)], sav.at[:, pl.ds(0, width - raw_b)]),
            ("down", down_hbm, down),
        )
    }
    loads["sav_tail"].start()
    loads["gain"].start()
    loads["sav"].start()
    loads["down"].start()
    for name, both, sources in (("kept_up", kept_up, (grad_hbm, up_hbm)),):
        loads[name] = pltpu.make_async_copy(both, both, sem(name))
        for source, first in zip(sources, (0, rows)):
            pltpu.make_async_copy(source, both.at[pl.ds(first, source.shape[0])], sem(name)).start()
    loads["len"].start()
    loads["fwd"].start()


    def remote(source, target, send, recv, **place):
        return pltpu.make_async_remote_copy(
            src_ref=source, dst_ref=target, send_sem=send, recv_sem=recv, device_id=place
        )

    def across(step, source, target, send, recv):
        return remote(source, target, send, recv, section=sec + step)

    raw_ups = across(1, up.at[mine, tail_f], raw_up.at[mine], sem("raw_up", "s"), sem("raw_up", "r"))
    raw_fwds = across(1, fwd.at[:, tail_f], raw_fwd, sem("out_f", "s"), sem("raw_fwd_r"))
    acts = across(1, act_out.at[own], pair.at[own, pl.ds(0, padded)], sem("act", "s"), sem("act", "r"))
    raw_downs = across(-1, gained.at[mine, tail_b], raw_down.at[mine], sem("raw_down", "s"), sem("raw_down", "r"))
    raw_savs = across(-1, sav.at[:, tail_b], raw_pair.at[0], sem("raw_sav_s"), sem("raw_pair_r"))
    raw_keeps = across(-1, kept.at[:, tail_b], raw_pair.at[1], sem("out_b", "s"), sem("raw_pair_r"))
    raw_pairs = across(-1, raw_pair, raw_pair, sem("raw_sav_s"), sem("raw_pair_r"))
    backs = across(-1, back_out.at[own], pair.at[own, pl.ds(padded, padded)], sem("back", "s"), sem("back", "r"))

    def relay(way, k):
        ref = (raw_up, raw_down)[way].at[mine]
        return remote(ref, ref, sem("relay", way, "s", k), sem("relay", way, "r", k), dp=(dp + k) % n_dp)

    first_rows = groups[0][1]

    def exchange_first():
        for k in range(n_ten - 1, 0, -1):
            place = {"tensor": peer(ten, k, bits)}
            remote(
                send_b.at[0, pl.ds(0, first_rows)], first_b.at[k - 1], sem("first", "s"), sem("first", "r"), **place
            ).start()
            remote(sq_out, sq_in.at[k - 1], sem("sq", "s"), sem("sq", "r"), **place).start()

    def exchange_b(start, size, g, p):
        for q in range(2):
            span = pl.ds(start + q * (size // 2), size // 2)
            remote(
                send_b.at[p, span], recv_b.at[p, span], sem("b_send"), sem("b", g, p), tensor=flip(ten, (q + p) % bits)
            ).start()

    def exchange_f(p):
        for q in range(2):
            span = pl.ds(q * (rows // 2), rows // 2)
            remote(
                send_f.at[p, span], recv_f.at[p, span], sem("f_send"), sem("f", p), tensor=flip(ten, (q + p) % bits)
            ).start()

    def arrived(target, recv):
        remote(target, target, sem("f_send"), recv, tensor=flip(ten, 0)).wait_recv()

    eye = lax.broadcasted_iota(jnp.int32, (rows, rows), 0) == lax.broadcasted_iota(jnp.int32, (rows, rows), 1)

    def to_row(column):
        return jnp.sum(jnp.where(eye, column, 0.0), axis=0, keepdims=True)

    def to_column(row):
        return jnp.sum(jnp.where(eye, row, 0.0), axis=1, keepdims=True)

    def spread(column, count):
        lane = lax.broadcasted_iota(jnp.int32, (column.shape[0], padded - rank), 1)
        result = jnp.zeros(lane.shape, F32)
        for i in range(count):
            piece = column.astype(BF16).astype(F32)
            result = jnp.where(lane == i, piece, result)
            column = column - piece
        return result.astype(BF16)

    loads["sav_tail"].wait()

    pl.semaphore_wait(barrier, len(near) + n_dp - 1 + jnp.where(sec > 0, 1, 0) + jnp.where(sec < n_sec - 1, 1, 0))
    if relayed:
        pl.semaphore_signal(far_sem, inc=1, device_id={"tensor": flip(ten, 0)})

    @pl.when(sec > 0)
    def _():
        raw_savs.start()

    for name in ("gain", "sav", "down"):
        loads[name].wait()
    square_s = jnp.zeros((rows, 1), F32)
    total_s = jnp.zeros((rows, rank), F32)
    for cols in columns:
        values = sav[:, cols].astype(F32)
        square_s += jnp.sum(values * values, axis=1, keepdims=True)
        scaled = down[:, cols] * gain[:, cols]
        gained[:, cols] = scaled
        total_s += contract_last(sav[:, cols], scaled)
    square_row = to_row(square_s)
    if bits:
        sq_out[...] = square_row

    @pl.when(sec > 0)
    def _():
        raw_downs.start()

    loads["len"].wait()
    loads["kept_up"].wait()

    @pl.when(sec < n_sec - 1)
    def _():
        raw_ups.start()

    position = lax.broadcasted_iota(jnp.int32, (rows, 1), 0)
    seq_rows = rows // n_seq
    limit = jnp.full((rows, 1), 0, jnp.int32)
    for i in range(n_seq):
        limit = jnp.where(position >= i * seq_rows, i * seq_rows + lens[0, i], limit)
    keep = position < limit
    total_g = jnp.zeros((rows, rank), F32)
    for cols in columns:
        total_g += contract_last(kept[:, cols], up[:, cols])
    total_b = jnp.concatenate([jnp.where(keep, total_g, 0.0), total_s], axis=1)
    acc_b[...] = total_b
    if bits:
        send_b[0] = total_b.astype(BF16)
        if relayed:
            pl.semaphore_wait(far_sem, 1)
        exchange_first()
        for g, (start, size) in list(enumerate(groups))[1:]:
            exchange_b(start, size, g, 0)

    loads["fwd"].wait()

    @pl.when(sec < n_sec - 1)
    def _():
        raw_fwds.start()

    for cols in columns[::-1]:
        kept[:, cols] = jnp.where(keep, kept[:, cols].astype(F32), 0.0).astype(BF16)

    @pl.when(sec > 0)
    def _():
        raw_keeps.start()

    total = jnp.zeros((rows, rank), F32)
    square_f = jnp.zeros((rows, 1), F32)
    for cols in columns:
        values = fwd[:, cols].astype(F32)
        square_f += jnp.sum(values * values, axis=1, keepdims=True)
        total += contract_last(fwd[:, cols], gained[:, cols])

    def begin_f(p, total, square_f):
        send_f[p, :, :rank] = total.astype(BF16)
        send_f[p, :, rank:] = spread(square_f, 3)
        exchange_f(p)

    if bits:
        begin_f(0, total, square_f)
    def step_b(p, chosen):
        for g, (start, size) in chosen:
            span = pl.ds(start, size)
            arrived(recv_b.at[p - 1, span], sem("b", g, p - 1))
            summed = acc_b[span] + recv_b[p - 1, span].astype(F32)
            acc_b[span] = summed
            send_b[p, span] = summed.astype(BF16)
            exchange_b(start, size, g, p)

    later = list(enumerate(groups))[1:]
    if bits > 1:
        step_b(1, later[:1])

    done_f = [slice(a, min(a + chunk, width - raw_f)) for a in range(0, width - raw_f, chunk)]
    done_b = [slice(a, min(a + chunk, width - raw_b)) for a in range(0, width - raw_b, chunk)]

    def shift(way, start, size, cols):
        source, target = ((out_f, next_in), (out_b, next_gr))[way]
        part_rows, span = pl.ds(start, size), pl.ds(cols.start, cols.stop - cols.start)
        name = ("out_f", "out_b")[way]
        return across(
            1 - 2 * way, source.at[part_rows, span], target.at[part_rows, span], sem(name, "s"), sem(name, "r")
        )

    if bits:
        arrived(sq_in, sem("sq", "r"))
        for k in range(1, n_ten):
            square_row += sq_in[k - 1]
    scale_s = lax.rsqrt(to_column(square_row) / full_width + EPSILON)
    acts_s, backs_s, tilts = [], [], []

    def give_back(start, size, back_rows, tilt, first):
        span = slice(start, start + size)
        for cols in done_b:
            normed = jnp.dot(back_rows, gained[:, cols], preferred_element_type=F32)
            out_b[span, cols] = (
                kept[span, cols].astype(F32)
                + normed
                - sav[span, cols].astype(F32) * tilt
            ).astype(BF16)
            if detour and first and start == groups[1][0]:
                send_middle(start, size, cols)
            elif first or cols in done_b[:1]:
                shift(1, start, size, cols).start()

    side = 2 * LANES
    cut = width - raw_b - 2 * side
    detour = bits == 2 and n_sec > 1 and len(groups) > 2 and n_dp > 1
    odd = dp % 2 == 1
    sender = jnp.logical_and(jnp.logical_and(sec == 1, ten == 0), odd)

    def side_way(bit):
        block = (pl.ds(*groups[1]), pl.ds(cut + bit * side, side))
        helped = remote(out_b.at[block], relief, sem("out_b", "s"), sem("relief", "r"), tensor=flip(ten, bit))
        given = remote(
            relief, next_gr.at[block], sem("relief", "s"), sem("out_b", "r"), section=sec - 1, tensor=flip(ten, bit)
        )
        return helped, given, jnp.logical_and(jnp.logical_and(sec == 1, ten == 1 << bit), odd)

    def send_middle(start, size, cols):
        @pl.when(sender)
        def _():
            if cols.start < cut:
                shift(1, start, size, slice(cols.start, min(cols.stop, cut))).start()
            for bit in range(2):
                if cols.start < cut + (bit + 1) * side <= cols.stop:
                    side_way(bit)[0].start()

        pl.when(jnp.logical_not(sender))(shift(1, start, size, cols).start)

    def send_late():
        start, size = groups[-1]
        for cols in done_b[1:]:
            shift(1, start, size, cols).start()

    for g, (start, size) in enumerate(groups):
        span = slice(start, start + size)
        if bits and g == 0:
            arrived(first_b, sem("first", "r"))
            summed = acc_b[span]
            for k in range(1, n_ten):
                summed += first_b[k - 1].astype(F32)
        elif bits:
            arrived(recv_b.at[bits - 1, pl.ds(start, size)], sem("b", g, bits - 1))
            summed = acc_b[span] + recv_b[bits - 1, span].astype(F32)
        else:
            summed = acc_b[span]
        own_scale = scale_s[span]
        slope = summed[:, :rank]
        rank_s = summed[:, rank:] * own_scale
        gate = jax.nn.sigmoid(rank_s)
        acts_s.append((rank_s * gate).astype(BF16))
        back = slope * (gate * (1.0 + rank_s * (1.0 - gate)))
        tilts.append(jnp.sum(back.astype(BF16).astype(F32) * rank_s, axis=1, keepdims=True) * (own_scale * own_scale / full_width))
        backs_s.append((back * own_scale).astype(BF16))
        if g == 0 and len(groups) > 1:
            @pl.when(sec > 0)
            def _():
                give_back(start, size, backs_s[0], tilts[0], True)
        if 0 < g < len(groups) - 1:
            @pl.when(jnp.logical_and(sec > 0, dp % 2 == 1))
            def _():
                give_back(start, size, backs_s[g], tilts[g], True)
        if g == 0:
            for p in range(1, bits):
                step_b(p, later[1:] if p == 1 else later)
            for p in range(1, bits):
                arrived(recv_f.at[p - 1], sem("f", p - 1))
                total += recv_f[p - 1, :, :rank].astype(F32)
                square_f += jnp.sum(recv_f[p - 1, :, rank:].astype(F32), axis=1, keepdims=True)
                begin_f(p, total, square_f)

    early = 1 if len(groups) > 1 else 0

    @pl.when(sec > 0)
    def _():
        for (start, size), back_rows, tilt in zip(groups, backs_s, tilts):
            back_out[start:start + size, :rank] = back_rows
            back_out[start:start + size, rank:] = spread(tilt, 2)
        backs.start()
        for g in range(early, len(groups) - 1):
            @pl.when(dp % 2 == 0)
            def _():
                give_back(*groups[g], backs_s[g], tilts[g], True)
        give_back(*groups[-1], backs_s[-1], tilts[-1], False)
        pl.when(dp % 2 == 0)(send_late)

    back_scaled = jnp.concatenate(backs_s, axis=0)
    act_s = jnp.concatenate(acts_s, axis=0)

    if bits:
        arrived(recv_f.at[bits - 1], sem("f", bits - 1))
        total += recv_f[bits - 1, :, :rank].astype(F32)
        square_f += jnp.sum(recv_f[bits - 1, :, rank:].astype(F32), axis=1, keepdims=True)
    rank_f = total * lax.rsqrt(square_f / full_width + EPSILON)
    act_f = (rank_f * jax.nn.sigmoid(rank_f)).astype(BF16)

    @pl.when(sec < n_sec - 1)
    def _():
        act_out[:, :rank] = act_f
        act_out[:, rank:] = jnp.zeros((rows, padded - rank), BF16)
        acts.start()
        for cols in done_f:
            grown = jnp.dot(act_f, up[:, cols], preferred_element_type=F32)
            out_f[:, cols] = (fwd[:, cols].astype(F32) + grown).astype(BF16)
            shift(0, 0, rows, cols).start()

    @pl.when(sec > 0)
    def _():
        raw_ups.wait_recv()
        for k in range(1, n_dp):
            relay(0, k).start()

    @pl.when(sec < n_sec - 1)
    def _():
        raw_downs.wait_recv()
        for k in range(1, n_dp):
            relay(1, k).start()

    def trade(k):
        target = (dp + k) % n_dp
        return remote(
            part.at[:, pl.ds(pl.multiple_of(target * share, share), share)], part_recv.at[k - 1],
            sem("trade", "s", k), sem("trade", "r", k), dp=target,
        )

    for cols in columns:
        part[0, :, cols] = (contract_rows(back_scaled, sav[:, cols]) * gain[:, cols].astype(F32)).astype(BF16)
        part[1, :, cols] = contract_rows(act_s, kept[:, cols]).astype(BF16)
    for k in range(1, n_dp):
        trade(k).start()

    if detour:
        for bit in range(2):
            helped, given, helper = side_way(bit)

            @pl.when(helper)
            def _():
                helped.wait_recv()
                given.start()

    @pl.when(sec == 0)
    def _():
        next_in[...] = jnp.zeros_like(next_in)

    @pl.when(sec == n_sec - 1)
    def _():
        next_gr[...] = jnp.zeros_like(next_gr)

    def gather(p):
        held_rows = quarter << p
        block = pl.ds(pl.multiple_of(ten // (1 << p) * held_rows, held_rows), held_rows)
        return remote(pair.at[block], pair.at[block], sem("all", "s", p), sem("all", "r", p), tensor=flip(ten, p))

    @pl.when(sec > 0)
    def _():
        acts.wait_recv()

    @pl.when(sec < n_sec - 1)
    def _():
        backs.wait_recv()

    if bits:
        gather(0).start()

    for k in range(1, n_dp):
        trade(k).wait()
    for i, out in enumerate((grad_down, grad_up)):
        for cols in columns:
            summed = part[i, mine, cols].astype(F32)
            for k in range(1, n_dp):
                summed += part_recv[k - 1, i, :, cols].astype(F32)
            out[:, cols] = (summed * (1.0 / n_dp)).astype(BF16)

    for p in range(bits):
        gather(p).wait()
        if p + 1 < bits:
            gather(p + 1).start()
        if p == 0:
            pl.when(jnp.logical_and(sec > 0, dp % 2 == 1))(send_late)

    @pl.when(sec > 0)
    def _():
        for k in range(1, n_dp):
            relay(0, k).wait()
        raw_fwds.wait_recv()
        for a in range(0, raw_f, chunk):
            b = min(a + chunk, raw_f)
            grown = jnp.dot(pair[:, :rank], raw_up[:, a:b], preferred_element_type=F32)
            next_in[:, width - raw_f + a:width - raw_f + b] = (raw_fwd[:, a:b].astype(F32) + grown).astype(BF16)

    @pl.when(sec < n_sec - 1)
    def _():
        for k in range(1, n_dp):
            relay(1, k).wait()
        raw_pairs.wait_recv()
        far_tilt = jnp.sum(pair[:, padded + rank:].astype(F32), axis=1, keepdims=True)
        for a in range(0, raw_b, chunk):
            b = min(a + chunk, raw_b)
            normed = jnp.dot(pair[:, padded:padded + rank], raw_down[:, a:b], preferred_element_type=F32)
            next_gr[:, width - raw_b + a:width - raw_b + b] = (
                raw_pair[1, :, a:b].astype(F32)
                + normed
                - raw_pair[0, :, a:b].astype(F32) * far_tilt
            ).astype(BF16)

    if bits:
        remote(sq_in, sq_in, sem("sq", "s"), sem("sq", "r"), tensor=flip(ten, 0)).wait_send()
        remote(first_b, first_b, sem("first", "s"), sem("first", "r"), tensor=flip(ten, 0)).wait_send()
        if len(groups) > 1:
            rest = send_b.at[:, pl.ds(first_rows, rows - first_rows)]
            remote(rest, rest, sem("b_send"), sem("first", "r"), tensor=flip(ten, 0)).wait_send()
        remote(send_f, recv_f, sem("f_send"), sem("f", 0), tensor=flip(ten, 0)).wait_send()

    if detour:
        for bit in range(2):
            helped, given, helper = side_way(bit)
            pl.when(helper)(given.wait_send)

    whole_f = across(1, fwd, out_f, sem("out_f", "s"), sem("out_f", "r"))
    whole_b = across(-1, kept, out_b, sem("out_b", "s"), sem("out_b", "r"))

    @pl.when(sec < n_sec - 1)
    def _():
        for copy in (raw_ups, acts, whole_f):
            copy.wait_send()

    @pl.when(sec > 0)
    def _():
        for copy in (raw_savs, raw_downs, backs, whole_b):
            copy.wait_send()

    @pl.when(sec < n_sec - 1)
    def _():
        shift(1, 0, rows, slice(0, width - raw_b)).wait_recv()

    @pl.when(sec > 0)
    def _():
        shift(0, 0, rows, slice(0, width - raw_f)).wait_recv()


def place(*refs):
    count = len(refs) // 2
    sems = refs[-1]
    copies = [pltpu.make_async_copy(refs[i], refs[count + i], sems.at[i]) for i in range(count)]
    for copy in copies:
        copy.start()
    for copy in copies:
        copy.wait()


def solution(mesh):
    n_sec, n_ten, n_dp = (mesh.shape[name] for name in ("section", "tensor", "dp"))

    def shards(forward_rows, saved_rows, output_grad, lengths, norm_gain, down_map, up_map):
        rows, width = forward_rows.shape[2:]
        rank = down_map.shape[1]
        n_seq = lengths.shape[2]
        share = rank // n_dp
        bits = n_ten.bit_length() - 1
        chunk = min(width, 4 * LANES)
        raw_f = int(width * RAW_FORWARD) // LANES * LANES
        raw_b = int(width * RAW_BACK) // LANES * LANES
        steps = max(bits, 1)
        padded = (rank + 3 + LANES - 1) // LANES * LANES
        vmem = pl.BlockSpec(memory_space=pltpu.VMEM)
        anywhere = pl.BlockSpec(memory_space=pl.ANY)
        flops = 7 * 2 * rows * rank * width
        dma = pltpu.SemaphoreType.DMA
        shapes = ((rows, width),) * 2 + ((share, width),) * 2
        results = pl.pallas_call(
            functools.partial(tick, (n_sec, n_ten, n_dp, chunk)),
            out_shape=tuple(pltpu.VMEM(shape, BF16) for shape in shapes),
            in_specs=[anywhere] * 7,
            out_specs=(vmem,) * 4,
            scratch_shapes=[
                pltpu.SMEM((1, n_seq), jnp.int32),
                pltpu.VMEM((1, width), BF16),
                pltpu.VMEM((rows, width), BF16),
                pltpu.VMEM((rows + rank, width), BF16),
                pltpu.VMEM((rows + rank, width), BF16),
                pltpu.VMEM((rows, width), BF16),
                pltpu.VMEM((rows, 2 * rank), F32),
                pltpu.VMEM((steps, rows, padded), BF16),
                pltpu.VMEM((steps, rows, padded), BF16),
                pltpu.VMEM((steps, rows, 2 * rank), BF16),
                pltpu.VMEM((steps, rows, 2 * rank), BF16),
                pltpu.VMEM((max(n_ten - 1, 1), row_groups(rows)[0][1], 2 * rank), BF16),
                pltpu.VMEM((rows, width), BF16),
                pltpu.VMEM((rows, width), BF16),
                pltpu.VMEM((2, rank, width), BF16),
                pltpu.VMEM((max(n_dp - 1, 1), 2, share, width), BF16),
                pltpu.VMEM((rows, padded), BF16),
                pltpu.VMEM((rows, padded), BF16),
                pltpu.VMEM((rows, 2 * padded), BF16),
                pltpu.VMEM((1, rows), F32),
                pltpu.VMEM((max(n_ten - 1, 1), 1, rows), F32),
                pltpu.VMEM((rows, raw_f), BF16),
                pltpu.VMEM((rank, raw_f), BF16),
                pltpu.VMEM((2, rows, raw_b), BF16),
                pltpu.VMEM((rank, raw_b), BF16),
                pltpu.VMEM((row_groups(rows)[1 % len(row_groups(rows))][1], 2 * LANES), BF16),
                dma((max(semaphores(len(row_groups(rows)), bits, n_dp).values()) + 1,)),
                pltpu.SemaphoreType.REGULAR,
            ],
            compiler_params=pltpu.CompilerParams(collective_id=0, has_side_effects=True),
            cost_estimate=pl.CostEstimate(
                flops=flops, bytes_accessed=16 * rows * width, transcendentals=4 * rows * rank
            ),
            name="tick",
        )(
            forward_rows[0, 0], saved_rows[0, 0], output_grad[0, 0], lengths[0], norm_gain, down_map[0], up_map[0]
        )
        next_inputs, next_grads, grad_down, grad_up = pl.pallas_call(
            place,
            out_shape=tuple(jax.ShapeDtypeStruct(shape, BF16) for shape in shapes),
            in_specs=[vmem] * 4,
            out_specs=(anywhere,) * 4,
            scratch_shapes=[dma((4,))],
            name="place",
        )(*[pltpu.with_memory_space_constraint(x, pltpu.VMEM) for x in results])
        return next_inputs[None, None], next_grads[None, None], grad_down[None], grad_up[None]

    row_spec = P("section", "dp", None, "tensor")
    map_spec = P("section", None, "tensor")
    part_spec = P("section", "dp", "tensor")
    return jax.shard_map(
        shards,
        mesh=mesh,
        in_specs=(row_spec, row_spec, row_spec, P("section", "dp"), P("section", "tensor"), map_spec, map_spec),
        out_specs=(row_spec, row_spec, part_spec, part_spec),
        check_vma=False,
    )
```

```python
import functools

import jax
import jax.numpy as jnp
from jax import lax
from jax.experimental import pallas as pl
from jax.experimental.pallas import tpu as pltpu
from jax.sharding import PartitionSpec as P

EPSILON = 1e-05
LANES = 128
RAW_FORWARD = 0.375
RAW_BACK = 0.125
F32 = jnp.float32
BF16 = jnp.bfloat16


def contract_last(left_side, right_side):
    return lax.dot_general(
        left_side, right_side, (((1,), (1,)), ((), ())), preferred_element_type=F32
    )


def contract_rows(left_side, right_side):
    return lax.dot_general(
        left_side, right_side, (((0,), (0,)), ((), ())), preferred_element_type=F32
    )


def flip(index, bit):
    step = 1 << bit
    return index + step * (1 - 2 * ((index // step) % 2))


def peer(index, k, bits):
    for bit in range(bits):
        if k >> bit & 1:
            index = flip(index, bit)
    return index


def row_groups(rows):
    sizes = (rows // 6, rows // 3, rows // 2) if rows % 192 == 0 else (rows,)
    starts = [sum(sizes[:i]) for i in range(len(sizes))]
    return list(zip(starts, sizes))


def semaphores(n_group, bits, n_dp):
    names = ["len", "gain", "fwd", "sav_tail", "sav", "down", "kept_up"]
    n_load = len(names)
    names += [(side, kind) for side in ("sq", "first") for kind in "sr"]
    names += [("b", g, p) for g in range(1, n_group) for p in range(bits)] + ["b_send"]
    names += [("f", p) for p in range(bits)] + ["f_send"]
    names += [(side, kind) for side in ("out_f", "out_b") for kind in "sr"]
    names += [(side, kind) for side in ("raw_up", "raw_down") for kind in "sr"] + [("act", "r"), ("back", "r")]
    names += ["raw_fwd_r", "raw_sav_s", "raw_pair_r", ("relief", "s"), ("relief", "r")]
    names += [("all", "r", p) for p in range(bits)] + [("trade", "r", k) for k in range(1, n_dp)]
    names += [("relay", way, "r", k) for way in range(2) for k in range(1, n_dp)]
    sends = [("act", "s"), ("back", "s")] + [("all", "s", p) for p in range(bits)]
    sends += [("trade", "s", k) for k in range(1, n_dp)]
    sends += [("relay", way, "s", k) for way in range(2) for k in range(1, n_dp)]
    names += sends[n_load:]
    index = {name: i for i, name in enumerate(names)}
    return index | {name: i for i, name in enumerate(sends[:n_load])}


def tick(sizes, fwd_hbm, sav_hbm, grad_hbm, len_hbm, gain_hbm, down_hbm, up_hbm,
         next_in, next_gr, grad_down, grad_up,
         lens, gain, fwd, sav_down, kept_up, gained,
         acc_b, send_f, recv_f, send_b, recv_b, first_b, out_f, out_b,
         part, part_recv, act_out, back_out, pair, sq_out, sq_in,
         raw_fwd, raw_up, raw_pair, raw_down, relief, sems, far_sem, up_sem):
    n_sec, n_ten, n_dp, chunk = sizes
    rows, width = fwd.shape
    rank = down_hbm.shape[0]
    sav, down = sav_down.at[pl.ds(0, rows)], sav_down.at[pl.ds(rows, rank)]
    kept, up = kept_up.at[pl.ds(0, rows)], kept_up.at[pl.ds(rows, rank)]
    padded = act_out.shape[1]
    full_width = width * n_ten
    n_seq = lens.shape[1]
    bits = n_ten.bit_length() - 1
    share = rank // n_dp
    quarter = rows // n_ten
    groups = row_groups(rows)
    columns = [slice(c, c + chunk) for c in range(0, width, chunk)]
    index = semaphores(len(groups), bits, n_dp)
    sec, ten, dp = lax.axis_index("section"), lax.axis_index("tensor"), lax.axis_index("dp")

    def sem(*name):
        return sems.at[index[name if len(name) > 1 else name[0]]]

    @pl.when(sec == 0)
    def _():
        pair[:, :padded] = jnp.zeros((rows, padded), BF16)

    @pl.when(sec == n_sec - 1)
    def _():
        pair[:, padded:] = jnp.zeros((rows, padded), BF16)

    barrier = pltpu.get_barrier_semaphore()
    relayed = bits == 2
    near = [1 << bit for bit in range(bits)] if relayed else range(1, n_ten)
    for k in near:
        pl.semaphore_signal(barrier, inc=1, device_id={"tensor": peer(ten, k, bits)})
    for k in range(1, n_dp):
        pl.semaphore_signal(barrier, inc=1, device_id={"dp": (dp + k) % n_dp})

    @pl.when(sec < n_sec - 1)
    def _():
        pl.semaphore_signal(barrier, inc=1, device_id={"section": sec + 1})

    raw_f, raw_b = raw_fwd.shape[1], raw_pair.shape[2]
    mine = pl.ds(pl.multiple_of(dp * share, share), share)
    own = pl.ds(pl.multiple_of(ten * quarter, quarter), quarter)
    tail_f, tail_b = pl.ds(width - raw_f, raw_f), pl.ds(width - raw_b, raw_b)
    loads = {
        name: pltpu.make_async_copy(source, target, sem(name))
        for name, source, target in (
            ("gain", gain_hbm, gain), ("len", len_hbm, lens), ("fwd", fwd_hbm, fwd),
            ("sav_tail", sav_hbm.at[:, tail_b], sav.at[:, tail_b]),
            ("sav", sav_hbm.at[:, pl.ds(0, width - raw_b)], sav.at[:, pl.ds(0, width - raw_b)]),
            ("down", down_hbm, down),
        )
    }
    loads["sav_tail"].start()
    loads["gain"].start()
    loads["sav"].start()
    loads["down"].start()
    for name, both, sources in (("kept_up", kept_up, (grad_hbm, up_hbm)),):
        loads[name] = pltpu.make_async_copy(both, both, sem(name))
        for source, first in zip(sources, (0, rows)):
            pltpu.make_async_copy(source, both.at[pl.ds(first, source.shape[0])], sem(name)).start()
    loads["len"].start()
    loads["fwd"].start()


    def remote(source, target, send, recv, **place):
        return pltpu.make_async_remote_copy(
            src_ref=source, dst_ref=target, send_sem=send, recv_sem=recv, device_id=place
        )

    def across(step, source, target, send, recv):
        return remote(source, target, send, recv, section=sec + step)

    raw_ups = across(1, up.at[mine, tail_f], raw_up.at[mine], sem("raw_up", "s"), sem("raw_up", "r"))
    raw_fwds = across(1, fwd.at[:, tail_f], raw_fwd, sem("out_f", "s"), sem("raw_fwd_r"))
    acts = across(1, act_out.at[own], pair.at[own, pl.ds(0, padded)], sem("act", "s"), sem("act", "r"))
    raw_downs = across(-1, gained.at[mine, tail_b], raw_down.at[mine], sem("raw_down", "s"), sem("raw_down", "r"))
    raw_savs = across(-1, sav.at[:, tail_b], raw_pair.at[0], sem("raw_sav_s"), sem("raw_pair_r"))
    raw_keeps = across(-1, kept.at[:, tail_b], raw_pair.at[1], sem("out_b", "s"), sem("raw_pair_r"))
    raw_pairs = across(-1, raw_pair, raw_pair, sem("raw_sav_s"), sem("raw_pair_r"))
    backs = across(-1, back_out.at[own], pair.at[own, pl.ds(padded, padded)], sem("back", "s"), sem("back", "r"))

    def relay(way, k):
        ref = (raw_up, raw_down)[way].at[mine]
        return remote(ref, ref, sem("relay", way, "s", k), sem("relay", way, "r", k), dp=(dp + k) % n_dp)

    first_rows = groups[0][1]

    def exchange_first():
        for k in range(n_ten - 1, 0, -1):
            place = {"tensor": peer(ten, k, bits)}
            remote(
                send_b.at[0, pl.ds(0, first_rows)], first_b.at[k - 1], sem("first", "s"), sem("first", "r"), **place
            ).start()
            remote(sq_out, sq_in.at[k - 1], sem("sq", "s"), sem("sq", "r"), **place).start()

    def exchange_b(start, size, g, p):
        for q in range(2):
            span = pl.ds(start + q * (size // 2), size // 2)
            remote(
                send_b.at[p, span], recv_b.at[p, span], sem("b_send"), sem("b", g, p), tensor=flip(ten, (q + p) % bits)
            ).start()

    def exchange_f(p):
        for q in range(2):
            span = pl.ds(q * (rows // 2), rows // 2)
            remote(
                send_f.at[p, span], recv_f.at[p, span], sem("f_send"), sem("f", p), tensor=flip(ten, (q + p) % bits)
            ).start()

    def arrived(target, recv):
        remote(target, target, sem("f_send"), recv, tensor=flip(ten, 0)).wait_recv()

    eye = lax.broadcasted_iota(jnp.int32, (rows, rows), 0) == lax.broadcasted_iota(jnp.int32, (rows, rows), 1)

    def to_row(column):
        return jnp.sum(jnp.where(eye, column, 0.0), axis=0, keepdims=True)

    def to_column(row):
        return jnp.sum(jnp.where(eye, row, 0.0), axis=1, keepdims=True)

    def spread(column, count):
        lane = lax.broadcasted_iota(jnp.int32, (column.shape[0], padded - rank), 1)
        result = jnp.zeros(lane.shape, F32)
        for i in range(count):
            piece = column.astype(BF16).astype(F32)
            result = jnp.where(lane == i, piece, result)
            column = column - piece
        return result.astype(BF16)

    loads["sav_tail"].wait()

    pl.semaphore_wait(barrier, len(near) + n_dp - 1 + jnp.where(sec > 0, 1, 0))

    @pl.when(sec > 0)
    def _():
        pl.semaphore_signal(up_sem, inc=1, device_id={"section": sec - 1})

    if relayed:
        pl.semaphore_signal(far_sem, inc=1, device_id={"tensor": flip(ten, 0)})

    @pl.when(sec > 0)
    def _():
        raw_savs.start()

    for name in ("gain", "sav", "down"):
        loads[name].wait()
    square_s = jnp.zeros((rows, 1), F32)
    total_s = jnp.zeros((rows, rank), F32)
    for cols in columns[::-1]:
        values = sav[:, cols].astype(F32)
        square_s += jnp.sum(values * values, axis=1, keepdims=True)
        scaled = down[:, cols] * gain[:, cols]
        gained[:, cols] = scaled
        total_s += contract_last(sav[:, cols], scaled)
    square_row = to_row(square_s)
    if bits:
        sq_out[...] = square_row

    @pl.when(sec > 0)
    def _():
        raw_downs.start()

    loads["len"].wait()
    loads["kept_up"].wait()

    position = lax.broadcasted_iota(jnp.int32, (rows, 1), 0)
    seq_rows = rows // n_seq
    limit = jnp.full((rows, 1), 0, jnp.int32)
    for i in range(n_seq):
        limit = jnp.where(position >= i * seq_rows, i * seq_rows + lens[0, i], limit)
    keep = position < limit
    total_g = jnp.zeros((rows, rank), F32)
    for cols in columns:
        total_g += contract_last(kept[:, cols], up[:, cols])
    total_b = jnp.concatenate([jnp.where(keep, total_g, 0.0), total_s], axis=1)
    acc_b[...] = total_b
    if bits:
        send_b[0] = total_b.astype(BF16)
        if relayed:
            pl.semaphore_wait(far_sem, 1)
        exchange_first()
        for g, (start, size) in list(enumerate(groups))[1:]:
            exchange_b(start, size, g, 0)

    loads["fwd"].wait()

    @pl.when(sec < n_sec - 1)
    def _():
        pl.semaphore_wait(up_sem, 1)
        raw_ups.start()
        raw_fwds.start()

    for cols in columns[::-1]:
        kept[:, cols] = jnp.where(keep, kept[:, cols].astype(F32), 0.0).astype(BF16)

    @pl.when(sec > 0)
    def _():
        raw_keeps.start()

    total = jnp.zeros((rows, rank), F32)
    square_f = jnp.zeros((rows, 1), F32)
    for cols in columns:
        values = fwd[:, cols].astype(F32)
        square_f += jnp.sum(values * values, axis=1, keepdims=True)
        total += contract_last(fwd[:, cols], gained[:, cols])

    def begin_f(p, total, square_f):
        send_f[p, :, :rank] = total.astype(BF16)
        send_f[p, :, rank:] = spread(square_f, 3)
        exchange_f(p)

    def step_b(p, chosen):
        for g, (start, size) in chosen:
            span = pl.ds(start, size)
            arrived(recv_b.at[p - 1, span], sem("b", g, p - 1))
            summed = acc_b[span] + recv_b[p - 1, span].astype(F32)
            acc_b[span] = summed
            send_b[p, span] = summed.astype(BF16)
            exchange_b(start, size, g, p)

    later = list(enumerate(groups))[1:]
    if bits > 1:
        step_b(1, later[:1])
    if bits:
        begin_f(0, total, square_f)

    done_f = [slice(a, min(a + chunk, width - raw_f)) for a in range(0, width - raw_f, chunk)]
    done_b = [slice(a, min(a + chunk, width - raw_b)) for a in range(0, width - raw_b, chunk)]

    def shift(way, start, size, cols):
        source, target = ((out_f, next_in), (out_b, next_gr))[way]
        part_rows, span = pl.ds(start, size), pl.ds(cols.start, cols.stop - cols.start)
        name = ("out_f", "out_b")[way]
        return across(
            1 - 2 * way, source.at[part_rows, span], target.at[part_rows, span], sem(name, "s"), sem(name, "r")
        )

    if bits:
        arrived(sq_in, sem("sq", "r"))
        for k in range(1, n_ten):
            square_row += sq_in[k - 1]
    scale_s = lax.rsqrt(to_column(square_row) / full_width + EPSILON)
    acts_s, backs_s, tilts = [], [], []

    def give_back(start, size, back_rows, tilt, first):
        span = slice(start, start + size)
        for cols in done_b:
            normed = jnp.dot(back_rows, gained[:, cols], preferred_element_type=F32)
            out_b[span, cols] = (
                kept[span, cols].astype(F32)
                + normed
                - sav[span, cols].astype(F32) * tilt
            ).astype(BF16)
            if detour and first and start == groups[1][0]:
                send_middle(start, size, cols)
            elif first or cols in done_b[:1]:
                shift(1, start, size, cols).start()

    side = 2 * LANES
    cut = width - raw_b - 2 * side
    detour = bits == 2 and n_sec > 1 and len(groups) > 2 and n_dp > 1
    odd = dp % 2 == 1
    sender = jnp.logical_and(jnp.logical_and(sec == 1, ten == 0), odd)

    def side_way(bit):
        block = (pl.ds(*groups[1]), pl.ds(cut + bit * side, side))
        helped = remote(out_b.at[block], relief, sem("out_b", "s"), sem("relief", "r"), tensor=flip(ten, bit))
        given = remote(
            relief, next_gr.at[block], sem("relief", "s"), sem("out_b", "r"), section=sec - 1, tensor=flip(ten, bit)
        )
        return helped, given, jnp.logical_and(jnp.logical_and(sec == 1, ten == 1 << bit), odd)

    def send_middle(start, size, cols):
        @pl.when(sender)
        def _():
            if cols.start < cut:
                shift(1, start, size, slice(cols.start, min(cols.stop, cut))).start()
            for bit in range(2):
                if cols.start < cut + (bit + 1) * side <= cols.stop:
                    side_way(bit)[0].start()

        pl.when(jnp.logical_not(sender))(shift(1, start, size, cols).start)

    def send_late():
        start, size = groups[-1]
        for cols in done_b[1:]:
            shift(1, start, size, cols).start()

    for g, (start, size) in enumerate(groups):
        span = slice(start, start + size)
        if bits and g == 0:
            arrived(first_b, sem("first", "r"))
            summed = acc_b[span]
            for k in range(1, n_ten):
                summed += first_b[k - 1].astype(F32)
        elif bits:
            arrived(recv_b.at[bits - 1, pl.ds(start, size)], sem("b", g, bits - 1))
            summed = acc_b[span] + recv_b[bits - 1, span].astype(F32)
        else:
            summed = acc_b[span]
        own_scale = scale_s[span]
        slope = summed[:, :rank]
        rank_s = summed[:, rank:] * own_scale
        gate = jax.nn.sigmoid(rank_s)
        acts_s.append((rank_s * gate).astype(BF16))
        back = slope * (gate * (1.0 + rank_s * (1.0 - gate)))
        tilts.append(jnp.sum(back.astype(BF16).astype(F32) * rank_s, axis=1, keepdims=True) * (own_scale * own_scale / full_width))
        backs_s.append((back * own_scale).astype(BF16))
        if g == 0 and len(groups) > 1:
            @pl.when(sec > 0)
            def _():
                give_back(start, size, backs_s[0], tilts[0], True)
        if 0 < g < len(groups) - 1:
            @pl.when(jnp.logical_and(sec > 0, dp % 2 == 1))
            def _():
                give_back(start, size, backs_s[g], tilts[g], True)
        if g == 0:
            for p in range(1, bits):
                step_b(p, later[1:] if p == 1 else later)
            for p in range(1, bits):
                arrived(recv_f.at[p - 1], sem("f", p - 1))
                total += recv_f[p - 1, :, :rank].astype(F32)
                square_f += jnp.sum(recv_f[p - 1, :, rank:].astype(F32), axis=1, keepdims=True)
                begin_f(p, total, square_f)

    early = 1 if len(groups) > 1 else 0

    @pl.when(sec > 0)
    def _():
        for (start, size), back_rows, tilt in zip(groups, backs_s, tilts):
            back_out[start:start + size, :rank] = back_rows
            back_out[start:start + size, rank:] = spread(tilt, 2)
        backs.start()
        for g in range(early, len(groups) - 1):
            @pl.when(dp % 2 == 0)
            def _():
                give_back(*groups[g], backs_s[g], tilts[g], True)
        give_back(*groups[-1], backs_s[-1], tilts[-1], False)
        pl.when(dp % 2 == 0)(send_late)

    back_scaled = jnp.concatenate(backs_s, axis=0)
    act_s = jnp.concatenate(acts_s, axis=0)

    if bits:
        arrived(recv_f.at[bits - 1], sem("f", bits - 1))
        total += recv_f[bits - 1, :, :rank].astype(F32)
        square_f += jnp.sum(recv_f[bits - 1, :, rank:].astype(F32), axis=1, keepdims=True)
    rank_f = total * lax.rsqrt(square_f / full_width + EPSILON)
    act_f = (rank_f * jax.nn.sigmoid(rank_f)).astype(BF16)

    @pl.when(sec < n_sec - 1)
    def _():
        act_out[:, :rank] = act_f
        act_out[:, rank:] = jnp.zeros((rows, padded - rank), BF16)
        acts.start()
        for cols in done_f:
            grown = jnp.dot(act_f, up[:, cols], preferred_element_type=F32)
            out_f[:, cols] = (fwd[:, cols].astype(F32) + grown).astype(BF16)
            shift(0, 0, rows, cols).start()

    @pl.when(sec > 0)
    def _():
        raw_ups.wait_recv()
        for k in range(1, n_dp):
            relay(0, k).start()

    @pl.when(sec < n_sec - 1)
    def _():
        raw_downs.wait_recv()
        for k in range(1, n_dp):
            relay(1, k).start()

    def trade(k):
        target = (dp + k) % n_dp
        return remote(
            part.at[:, pl.ds(pl.multiple_of(target * share, share), share)], part_recv.at[k - 1],
            sem("trade", "s", k), sem("trade", "r", k), dp=target,
        )

    for cols in columns:
        part[0, :, cols] = (contract_rows(back_scaled, sav[:, cols]) * gain[:, cols].astype(F32)).astype(BF16)
        part[1, :, cols] = contract_rows(act_s, kept[:, cols]).astype(BF16)
    for k in range(1, n_dp):
        trade(k).start()

    if detour:
        for bit in range(2):
            helped, given, helper = side_way(bit)

            @pl.when(helper)
            def _():
                helped.wait_recv()
                given.start()

    @pl.when(sec == 0)
    def _():
        next_in[...] = jnp.zeros_like(next_in)

    @pl.when(sec == n_sec - 1)
    def _():
        next_gr[...] = jnp.zeros_like(next_gr)

    def gather(p):
        held_rows = quarter << p
        block = pl.ds(pl.multiple_of(ten // (1 << p) * held_rows, held_rows), held_rows)
        return remote(pair.at[block], pair.at[block], sem("all", "s", p), sem("all", "r", p), tensor=flip(ten, p))

    @pl.when(sec > 0)
    def _():
        acts.wait_recv()

    @pl.when(sec < n_sec - 1)
    def _():
        backs.wait_recv()

    if bits:
        gather(0).start()

    for k in range(1, n_dp):
        trade(k).wait()
    for i, out in enumerate((grad_down, grad_up)):
        for cols in columns:
            summed = part[i, mine, cols].astype(F32)
            for k in range(1, n_dp):
                summed += part_recv[k - 1, i, :, cols].astype(F32)
            out[:, cols] = (summed * (1.0 / n_dp)).astype(BF16)

    for p in range(bits):
        gather(p).wait()
        if p + 1 < bits:
            gather(p + 1).start()
        if p == 0:
            pl.when(jnp.logical_and(sec > 0, dp % 2 == 1))(send_late)

    @pl.when(sec > 0)
    def _():
        for k in range(1, n_dp):
            relay(0, k).wait()
        raw_fwds.wait_recv()
        for a in range(0, raw_f, chunk):
            b = min(a + chunk, raw_f)
            grown = jnp.dot(pair[:, :rank], raw_up[:, a:b], preferred_element_type=F32)
            next_in[:, width - raw_f + a:width - raw_f + b] = (raw_fwd[:, a:b].astype(F32) + grown).astype(BF16)

    @pl.when(sec < n_sec - 1)
    def _():
        for k in range(1, n_dp):
            relay(1, k).wait()
        raw_pairs.wait_recv()
        far_tilt = jnp.sum(pair[:, padded + rank:].astype(F32), axis=1, keepdims=True)
        for a in range(0, raw_b, chunk):
            b = min(a + chunk, raw_b)
            normed = jnp.dot(pair[:, padded:padded + rank], raw_down[:, a:b], preferred_element_type=F32)
            next_gr[:, width - raw_b + a:width - raw_b + b] = (
                raw_pair[1, :, a:b].astype(F32)
                + normed
                - raw_pair[0, :, a:b].astype(F32) * far_tilt
            ).astype(BF16)

    if bits:
        remote(sq_in, sq_in, sem("sq", "s"), sem("sq", "r"), tensor=flip(ten, 0)).wait_send()
        remote(first_b, first_b, sem("first", "s"), sem("first", "r"), tensor=flip(ten, 0)).wait_send()
        if len(groups) > 1:
            rest = send_b.at[:, pl.ds(first_rows, rows - first_rows)]
            remote(rest, rest, sem("b_send"), sem("first", "r"), tensor=flip(ten, 0)).wait_send()
        remote(send_f, recv_f, sem("f_send"), sem("f", 0), tensor=flip(ten, 0)).wait_send()

    if detour:
        for bit in range(2):
            helped, given, helper = side_way(bit)
            pl.when(helper)(given.wait_send)

    whole_f = across(1, fwd, out_f, sem("out_f", "s"), sem("out_f", "r"))
    whole_b = across(-1, kept, out_b, sem("out_b", "s"), sem("out_b", "r"))

    @pl.when(sec < n_sec - 1)
    def _():
        for copy in (raw_ups, acts, whole_f):
            copy.wait_send()

    @pl.when(sec > 0)
    def _():
        for copy in (raw_savs, raw_downs, backs, whole_b):
            copy.wait_send()

    @pl.when(sec < n_sec - 1)
    def _():
        shift(1, 0, rows, slice(0, width - raw_b)).wait_recv()

    @pl.when(sec > 0)
    def _():
        shift(0, 0, rows, slice(0, width - raw_f)).wait_recv()


def place(*refs):
    count = len(refs) // 2
    sems = refs[-1]
    copies = [pltpu.make_async_copy(refs[i], refs[count + i], sems.at[i]) for i in range(count)]
    for copy in copies:
        copy.start()
    for copy in copies:
        copy.wait()


def solution(mesh):
    n_sec, n_ten, n_dp = (mesh.shape[name] for name in ("section", "tensor", "dp"))

    def shards(forward_rows, saved_rows, output_grad, lengths, norm_gain, down_map, up_map):
        rows, width = forward_rows.shape[2:]
        rank = down_map.shape[1]
        n_seq = lengths.shape[2]
        share = rank // n_dp
        bits = n_ten.bit_length() - 1
        chunk = min(width, 4 * LANES)
        raw_f = int(width * RAW_FORWARD) // LANES * LANES
        raw_b = int(width * RAW_BACK) // LANES * LANES
        steps = max(bits, 1)
        padded = (rank + 3 + LANES - 1) // LANES * LANES
        vmem = pl.BlockSpec(memory_space=pltpu.VMEM)
        anywhere = pl.BlockSpec(memory_space=pl.ANY)
        flops = 7 * 2 * rows * rank * width
        dma = pltpu.SemaphoreType.DMA
        shapes = ((rows, width),) * 2 + ((share, width),) * 2
        results = pl.pallas_call(
            functools.partial(tick, (n_sec, n_ten, n_dp, chunk)),
            out_shape=tuple(pltpu.VMEM(shape, BF16) for shape in shapes),
            in_specs=[anywhere] * 7,
            out_specs=(vmem,) * 4,
            scratch_shapes=[
                pltpu.SMEM((1, n_seq), jnp.int32),
                pltpu.VMEM((1, width), BF16),
                pltpu.VMEM((rows, width), BF16),
                pltpu.VMEM((rows + rank, width), BF16),
                pltpu.VMEM((rows + rank, width), BF16),
                pltpu.VMEM((rows, width), BF16),
                pltpu.VMEM((rows, 2 * rank), F32),
                pltpu.VMEM((steps, rows, padded), BF16),
                pltpu.VMEM((steps, rows, padded), BF16),
                pltpu.VMEM((steps, rows, 2 * rank), BF16),
                pltpu.VMEM((steps, rows, 2 * rank), BF16),
                pltpu.VMEM((max(n_ten - 1, 1), row_groups(rows)[0][1], 2 * rank), BF16),
                pltpu.VMEM((rows, width), BF16),
                pltpu.VMEM((rows, width), BF16),
                pltpu.VMEM((2, rank, width), BF16),
                pltpu.VMEM((max(n_dp - 1, 1), 2, share, width), BF16),
                pltpu.VMEM((rows, padded), BF16),
                pltpu.VMEM((rows, padded), BF16),
                pltpu.VMEM((rows, 2 * padded), BF16),
                pltpu.VMEM((1, rows), F32),
                pltpu.VMEM((max(n_ten - 1, 1), 1, rows), F32),
                pltpu.VMEM((rows, raw_f), BF16),
                pltpu.VMEM((rank, raw_f), BF16),
                pltpu.VMEM((2, rows, raw_b), BF16),
                pltpu.VMEM((rank, raw_b), BF16),
                pltpu.VMEM((row_groups(rows)[1 % len(row_groups(rows))][1], 2 * LANES), BF16),
                dma((max(semaphores(len(row_groups(rows)), bits, n_dp).values()) + 1,)),
                pltpu.SemaphoreType.REGULAR,
                pltpu.SemaphoreType.REGULAR,
            ],
            compiler_params=pltpu.CompilerParams(collective_id=0, has_side_effects=True),
            cost_estimate=pl.CostEstimate(
                flops=flops, bytes_accessed=16 * rows * width, transcendentals=4 * rows * rank
            ),
            name="tick",
        )(
            forward_rows[0, 0], saved_rows[0, 0], output_grad[0, 0], lengths[0], norm_gain, down_map[0], up_map[0]
        )
        next_inputs, next_grads, grad_down, grad_up = pl.pallas_call(
            place,
            out_shape=tuple(jax.ShapeDtypeStruct(shape, BF16) for shape in shapes),
            in_specs=[vmem] * 4,
            out_specs=(anywhere,) * 4,
            scratch_shapes=[dma((4,))],
            name="place",
        )(*[pltpu.with_memory_space_constraint(x, pltpu.VMEM) for x in results])
        return next_inputs[None, None], next_grads[None, None], grad_down[None], grad_up[None]

    row_spec = P("section", "dp", None, "tensor")
    map_spec = P("section", None, "tensor")
    part_spec = P("section", "dp", "tensor")
    return jax.shard_map(
        shards,
        mesh=mesh,
        in_specs=(row_spec, row_spec, row_spec, P("section", "dp"), P("section", "tensor"), map_spec, map_spec),
        out_specs=(row_spec, row_spec, part_spec, part_spec),
        check_vma=False,
    )
```

```python
import functools

import jax
import jax.numpy as jnp
from jax import lax
from jax.experimental import pallas as pl
from jax.experimental.pallas import tpu as pltpu
from jax.sharding import PartitionSpec as P

EPSILON = 1e-05
LANES = 128
RAW_FORWARD = 0.375
RAW_BACK = 0.125
F32 = jnp.float32
BF16 = jnp.bfloat16


def contract_last(left_side, right_side):
    return lax.dot_general(
        left_side, right_side, (((1,), (1,)), ((), ())), preferred_element_type=F32
    )


def contract_rows(left_side, right_side):
    return lax.dot_general(
        left_side, right_side, (((0,), (0,)), ((), ())), preferred_element_type=F32
    )


def flip(index, bit):
    step = 1 << bit
    return index + step * (1 - 2 * ((index // step) % 2))


def peer(index, k, bits):
    for bit in range(bits):
        if k >> bit & 1:
            index = flip(index, bit)
    return index


def row_groups(rows):
    sizes = (rows // 6, rows // 3, rows // 2) if rows % 192 == 0 else (rows,)
    starts = [sum(sizes[:i]) for i in range(len(sizes))]
    return list(zip(starts, sizes))


def semaphores(n_group, bits, n_dp):
    names = ["len", "gain", "fwd", "sav_tail", "sav", "down", "kept_up"]
    n_load = len(names)
    names += [(side, kind) for side in ("sq", "first") for kind in "sr"]
    names += [("b", g, p) for g in range(1, n_group) for p in range(bits)] + ["b_send"]
    names += [("f", p) for p in range(bits)] + ["f_send"]
    names += [(side, kind) for side in ("out_f", "out_b") for kind in "sr"]
    names += [(side, kind) for side in ("raw_up", "raw_down") for kind in "sr"] + [("act", "r"), ("back", "r")]
    names += ["raw_fwd_r", "raw_sav_s", "raw_pair_r", ("relief", "s"), ("relief", "r")]
    names += [("all", "r", p) for p in range(bits)] + [("trade", "r", k) for k in range(1, n_dp)]
    names += [("relay", way, "r", k) for way in range(2) for k in range(1, n_dp)]
    sends = [("act", "s"), ("back", "s")] + [("all", "s", p) for p in range(bits)]
    sends += [("trade", "s", k) for k in range(1, n_dp)]
    sends += [("relay", way, "s", k) for way in range(2) for k in range(1, n_dp)]
    names += sends[n_load:]
    index = {name: i for i, name in enumerate(names)}
    return index | {name: i for i, name in enumerate(sends[:n_load])}


def tick(sizes, fwd_hbm, sav_hbm, grad_hbm, len_hbm, gain_hbm, down_hbm, up_hbm,
         next_in, next_gr, grad_down, grad_up,
         lens, gain, fwd, sav_down, kept_up, gained,
         acc_b, send_f, recv_f, send_b, recv_b, first_b, out_f, out_b,
         part, part_recv, act_out, back_out, pair, sq_out, sq_in,
         raw_fwd, raw_up, raw_pair, raw_down, relief, sems, far_sem, up_sem):
    n_sec, n_ten, n_dp, chunk = sizes
    rows, width = fwd.shape
    rank = down_hbm.shape[0]
    sav, down = sav_down.at[pl.ds(0, rows)], sav_down.at[pl.ds(rows, rank)]
    kept, up = kept_up.at[pl.ds(0, rows)], kept_up.at[pl.ds(rows, rank)]
    padded = act_out.shape[1]
    full_width = width * n_ten
    n_seq = lens.shape[1]
    bits = n_ten.bit_length() - 1
    share = rank // n_dp
    quarter = rows // n_ten
    groups = row_groups(rows)
    columns = [slice(c, c + chunk) for c in range(0, width, chunk)]
    index = semaphores(len(groups), bits, n_dp)
    sec, ten, dp = lax.axis_index("section"), lax.axis_index("tensor"), lax.axis_index("dp")

    def sem(*name):
        return sems.at[index[name if len(name) > 1 else name[0]]]

    @pl.when(sec == 0)
    def _():
        pair[:, :padded] = jnp.zeros((rows, padded), BF16)

    @pl.when(sec == n_sec - 1)
    def _():
        pair[:, padded:] = jnp.zeros((rows, padded), BF16)

    barrier = pltpu.get_barrier_semaphore()
    relayed = bits == 2
    near = [1 << bit for bit in range(bits)] if relayed else range(1, n_ten)
    for k in near:
        pl.semaphore_signal(barrier, inc=1, device_id={"tensor": peer(ten, k, bits)})
    for k in range(1, n_dp):
        pl.semaphore_signal(barrier, inc=1, device_id={"dp": (dp + k) % n_dp})

    @pl.when(sec < n_sec - 1)
    def _():
        pl.semaphore_signal(barrier, inc=1, device_id={"section": sec + 1})

    raw_f, raw_b = raw_fwd.shape[1], raw_pair.shape[2]
    mine = pl.ds(pl.multiple_of(dp * share, share), share)
    own = pl.ds(pl.multiple_of(ten * quarter, quarter), quarter)
    tail_f, tail_b = pl.ds(width - raw_f, raw_f), pl.ds(width - raw_b, raw_b)
    loads = {
        name: pltpu.make_async_copy(source, target, sem(name))
        for name, source, target in (
            ("gain", gain_hbm, gain), ("len", len_hbm, lens), ("fwd", fwd_hbm, fwd),
            ("sav_tail", sav_hbm.at[:, tail_b], sav.at[:, tail_b]),
            ("sav", sav_hbm.at[:, pl.ds(0, width - raw_b)], sav.at[:, pl.ds(0, width - raw_b)]),
            ("down", down_hbm, down),
        )
    }
    loads["sav_tail"].start()
    loads["gain"].start()
    loads["sav"].start()
    loads["down"].start()
    for name, both, sources in (("kept_up", kept_up, (grad_hbm, up_hbm)),):
        loads[name] = pltpu.make_async_copy(both, both, sem(name))
        for source, first in zip(sources, (0, rows)):
            pltpu.make_async_copy(source, both.at[pl.ds(first, source.shape[0])], sem(name)).start()
    loads["len"].start()
    loads["fwd"].start()


    def remote(source, target, send, recv, **place):
        return pltpu.make_async_remote_copy(
            src_ref=source, dst_ref=target, send_sem=send, recv_sem=recv, device_id=place
        )

    def across(step, source, target, send, recv):
        return remote(source, target, send, recv, section=sec + step)

    raw_ups = across(1, up.at[mine, tail_f], raw_up.at[mine], sem("raw_up", "s"), sem("raw_up", "r"))
    raw_fwds = across(1, fwd.at[:, tail_f], raw_fwd, sem("out_f", "s"), sem("raw_fwd_r"))
    acts = across(1, act_out.at[own], pair.at[own, pl.ds(0, padded)], sem("act", "s"), sem("act", "r"))
    raw_downs = across(-1, gained.at[mine, tail_b], raw_down.at[mine], sem("raw_down", "s"), sem("raw_down", "r"))
    raw_savs = across(-1, sav.at[:, tail_b], raw_pair.at[0], sem("raw_sav_s"), sem("raw_pair_r"))
    raw_keeps = across(-1, kept.at[:, tail_b], raw_pair.at[1], sem("out_b", "s"), sem("raw_pair_r"))
    raw_pairs = across(-1, raw_pair, raw_pair, sem("raw_sav_s"), sem("raw_pair_r"))
    backs = across(-1, back_out.at[own], pair.at[own, pl.ds(padded, padded)], sem("back", "s"), sem("back", "r"))

    def relay(way, k):
        ref = (raw_up, raw_down)[way].at[mine]
        return remote(ref, ref, sem("relay", way, "s", k), sem("relay", way, "r", k), dp=(dp + k) % n_dp)

    first_rows = groups[0][1]

    def exchange_first():
        for k in range(n_ten - 1, 0, -1):
            place = {"tensor": peer(ten, k, bits)}
            remote(
                send_b.at[0, pl.ds(0, first_rows)], first_b.at[k - 1], sem("first", "s"), sem("first", "r"), **place
            ).start()
            remote(sq_out, sq_in.at[k - 1], sem("sq", "s"), sem("sq", "r"), **place).start()

    def exchange_b(start, size, g, p):
        for q in range(2):
            span = pl.ds(start + q * (size // 2), size // 2)
            remote(
                send_b.at[p, span], recv_b.at[p, span], sem("b_send"), sem("b", g, p), tensor=flip(ten, (q + p) % bits)
            ).start()

    def exchange_f(p):
        for q in range(2):
            span = pl.ds(q * (rows // 2), rows // 2)
            remote(
                send_f.at[p, span], recv_f.at[p, span], sem("f_send"), sem("f", p), tensor=flip(ten, (q + p) % bits)
            ).start()

    def arrived(target, recv):
        remote(target, target, sem("f_send"), recv, tensor=flip(ten, 0)).wait_recv()

    eye = lax.broadcasted_iota(jnp.int32, (rows, rows), 0) == lax.broadcasted_iota(jnp.int32, (rows, rows), 1)

    def to_row(column):
        return jnp.sum(jnp.where(eye, column, 0.0), axis=0, keepdims=True)

    def to_column(row):
        return jnp.sum(jnp.where(eye, row, 0.0), axis=1, keepdims=True)

    def spread(column, count):
        lane = lax.broadcasted_iota(jnp.int32, (column.shape[0], padded - rank), 1)
        result = jnp.zeros(lane.shape, F32)
        for i in range(count):
            piece = column.astype(BF16).astype(F32)
            result = jnp.where(lane == i, piece, result)
            column = column - piece
        return result.astype(BF16)

    loads["sav_tail"].wait()

    pl.semaphore_wait(barrier, len(near) + n_dp - 1 + jnp.where(sec > 0, 1, 0))

    @pl.when(sec > 0)
    def _():
        pl.semaphore_signal(up_sem, inc=1, device_id={"section": sec - 1})

    if relayed:
        pl.semaphore_signal(far_sem, inc=1, device_id={"tensor": flip(ten, 0)})

    @pl.when(sec > 0)
    def _():
        raw_savs.start()

    for name in ("gain", "sav", "down"):
        loads[name].wait()
    square_s = jnp.zeros((rows, 1), F32)
    total_s = jnp.zeros((rows, rank), F32)
    for cols in columns[::-1]:
        values = sav[:, cols].astype(F32)
        square_s += jnp.sum(values * values, axis=1, keepdims=True)
        scaled = down[:, cols] * gain[:, cols]
        gained[:, cols] = scaled
        total_s += contract_last(sav[:, cols], scaled)
    square_row = to_row(square_s)
    if bits:
        sq_out[...] = square_row

    @pl.when(sec > 0)
    def _():
        raw_downs.start()

    loads["len"].wait()
    loads["kept_up"].wait()

    position = lax.broadcasted_iota(jnp.int32, (rows, 1), 0)
    seq_rows = rows // n_seq
    limit = jnp.full((rows, 1), 0, jnp.int32)
    for i in range(n_seq):
        limit = jnp.where(position >= i * seq_rows, i * seq_rows + lens[0, i], limit)
    keep = position < limit
    total_g = jnp.zeros((rows, rank), F32)
    for cols in columns:
        total_g += contract_last(kept[:, cols], up[:, cols])
    total_b = jnp.concatenate([jnp.where(keep, total_g, 0.0), total_s], axis=1)
    acc_b[...] = total_b
    if bits:
        send_b[0] = total_b.astype(BF16)
        if relayed:
            pl.semaphore_wait(far_sem, 1)
        exchange_first()
        for g, (start, size) in list(enumerate(groups))[1:]:
            exchange_b(start, size, g, 0)

    loads["fwd"].wait()

    @pl.when(sec < n_sec - 1)
    def _():
        pl.semaphore_wait(up_sem, 1)
        raw_ups.start()
        raw_fwds.start()

    for cols in columns[::-1]:
        kept[:, cols] = jnp.where(keep, kept[:, cols].astype(F32), 0.0).astype(BF16)

    @pl.when(sec > 0)
    def _():
        raw_keeps.start()

    total = jnp.zeros((rows, rank), F32)
    square_f = jnp.zeros((rows, 1), F32)
    for cols in columns:
        values = fwd[:, cols].astype(F32)
        square_f += jnp.sum(values * values, axis=1, keepdims=True)
        total += contract_last(fwd[:, cols], gained[:, cols])

    def begin_f(p, total, square_f):
        send_f[p, :, :rank] = total.astype(BF16)
        send_f[p, :, rank:] = spread(square_f, 3)
        exchange_f(p)

    def step_b(p, chosen):
        for g, (start, size) in chosen:
            span = pl.ds(start, size)
            arrived(recv_b.at[p - 1, span], sem("b", g, p - 1))
            summed = acc_b[span] + recv_b[p - 1, span].astype(F32)
            acc_b[span] = summed
            send_b[p, span] = summed.astype(BF16)
            exchange_b(start, size, g, p)

    later = list(enumerate(groups))[1:]
    if bits > 1:
        step_b(1, later[:1])
    if bits:
        begin_f(0, total, square_f)

    done_f = [slice(a, min(a + chunk, width - raw_f)) for a in range(0, width - raw_f, chunk)]
    done_b = [slice(a, min(a + chunk, width - raw_b)) for a in range(0, width - raw_b, chunk)]

    def shift(way, start, size, cols):
        source, target = ((out_f, next_in), (out_b, next_gr))[way]
        part_rows, span = pl.ds(start, size), pl.ds(cols.start, cols.stop - cols.start)
        name = ("out_f", "out_b")[way]
        return across(
            1 - 2 * way, source.at[part_rows, span], target.at[part_rows, span], sem(name, "s"), sem(name, "r")
        )

    if bits:
        arrived(sq_in, sem("sq", "r"))
        for k in range(1, n_ten):
            square_row += sq_in[k - 1]
    scale_s = lax.rsqrt(to_column(square_row) / full_width + EPSILON)
    acts_s, backs_s, tilts = [], [], []

    def give_back(start, size, back_rows, tilt, first):
        span = slice(start, start + size)
        for cols in done_b:
            normed = jnp.dot(back_rows, gained[:, cols], preferred_element_type=F32)
            out_b[span, cols] = (
                kept[span, cols].astype(F32)
                + normed
                - sav[span, cols].astype(F32) * tilt
            ).astype(BF16)
            if detour and first and start == groups[1][0]:
                send_middle(start, size, cols)
            elif first or cols in done_b[:1]:
                shift(1, start, size, cols).start()

    side = 2 * LANES
    cut = width - raw_b - 3 * side
    detour = bits == 2 and n_sec > 1 and len(groups) > 2 and n_dp > 1 and cut > 0
    odd = dp % 2 == 1
    sender = jnp.logical_and(ten == 0, odd)

    def side_way(k):
        block = (pl.ds(*groups[1]), pl.ds(cut + (k - 1) * side, side))
        place = peer(ten, k, bits)
        helped = remote(out_b.at[block], relief, sem("out_b", "s"), sem("relief", "r"), tensor=place)
        given = remote(
            relief, next_gr.at[block], sem("relief", "s"), sem("out_b", "r"), section=sec - 1, tensor=place
        )
        wanted = sec > 0 if k == 3 else sec == 1
        return helped, given, jnp.logical_and(jnp.logical_and(wanted, ten == k), odd)

    def send_middle(start, size, cols):
        @pl.when(sender)
        def _():
            if cols.start < cut:
                shift(1, start, size, slice(cols.start, min(cols.stop, cut))).start()
            for k in range(1, 4):
                first = cut + (k - 1) * side
                if cols.start < first + side <= cols.stop:
                    if k == 3:
                        side_way(k)[0].start()
                    else:
                        pl.when(sec == 1)(side_way(k)[0].start)
                        pl.when(sec > 1)(shift(1, start, size, slice(first, first + side)).start)

        pl.when(jnp.logical_not(sender))(shift(1, start, size, cols).start)

    def send_late():
        start, size = groups[-1]
        for cols in done_b[1:]:
            shift(1, start, size, cols).start()

    for g, (start, size) in enumerate(groups):
        span = slice(start, start + size)
        if bits and g == 0:
            arrived(first_b, sem("first", "r"))
            summed = acc_b[span]
            for k in range(1, n_ten):
                summed += first_b[k - 1].astype(F32)
        elif bits:
            arrived(recv_b.at[bits - 1, pl.ds(start, size)], sem("b", g, bits - 1))
            summed = acc_b[span] + recv_b[bits - 1, span].astype(F32)
        else:
            summed = acc_b[span]
        own_scale = scale_s[span]
        slope = summed[:, :rank]
        rank_s = summed[:, rank:] * own_scale
        gate = jax.nn.sigmoid(rank_s)
        acts_s.append((rank_s * gate).astype(BF16))
        back = slope * (gate * (1.0 + rank_s * (1.0 - gate)))
        tilts.append(jnp.sum(back.astype(BF16).astype(F32) * rank_s, axis=1, keepdims=True) * (own_scale * own_scale / full_width))
        backs_s.append((back * own_scale).astype(BF16))
        if g == 0 and len(groups) > 1:
            @pl.when(sec > 0)
            def _():
                give_back(start, size, backs_s[0], tilts[0], True)
        if 0 < g < len(groups) - 1:
            @pl.when(jnp.logical_and(sec > 0, dp % 2 == 1))
            def _():
                give_back(start, size, backs_s[g], tilts[g], True)
        if g == 0:
            for p in range(1, bits):
                step_b(p, later[1:] if p == 1 else later)
            for p in range(1, bits):
                arrived(recv_f.at[p - 1], sem("f", p - 1))
                total += recv_f[p - 1, :, :rank].astype(F32)
                square_f += jnp.sum(recv_f[p - 1, :, rank:].astype(F32), axis=1, keepdims=True)
                begin_f(p, total, square_f)

    early = 1 if len(groups) > 1 else 0

    @pl.when(sec > 0)
    def _():
        for (start, size), back_rows, tilt in zip(groups, backs_s, tilts):
            back_out[start:start + size, :rank] = back_rows
            back_out[start:start + size, rank:] = spread(tilt, 2)
        backs.start()
        for g in range(early, len(groups) - 1):
            @pl.when(dp % 2 == 0)
            def _():
                give_back(*groups[g], backs_s[g], tilts[g], True)
        give_back(*groups[-1], backs_s[-1], tilts[-1], False)
        pl.when(dp % 2 == 0)(send_late)

    back_scaled = jnp.concatenate(backs_s, axis=0)
    act_s = jnp.concatenate(acts_s, axis=0)

    if bits:
        arrived(recv_f.at[bits - 1], sem("f", bits - 1))
        total += recv_f[bits - 1, :, :rank].astype(F32)
        square_f += jnp.sum(recv_f[bits - 1, :, rank:].astype(F32), axis=1, keepdims=True)
    rank_f = total * lax.rsqrt(square_f / full_width + EPSILON)
    act_f = (rank_f * jax.nn.sigmoid(rank_f)).astype(BF16)

    @pl.when(sec < n_sec - 1)
    def _():
        act_out[:, :rank] = act_f
        act_out[:, rank:] = jnp.zeros((rows, padded - rank), BF16)
        acts.start()
        for cols in done_f:
            grown = jnp.dot(act_f, up[:, cols], preferred_element_type=F32)
            out_f[:, cols] = (fwd[:, cols].astype(F32) + grown).astype(BF16)
            shift(0, 0, rows, cols).start()

    @pl.when(sec > 0)
    def _():
        raw_ups.wait_recv()
        for k in range(1, n_dp):
            relay(0, k).start()

    @pl.when(sec < n_sec - 1)
    def _():
        raw_downs.wait_recv()
        for k in range(1, n_dp):
            relay(1, k).start()

    def trade(k):
        target = (dp + k) % n_dp
        return remote(
            part.at[:, pl.ds(pl.multiple_of(target * share, share), share)], part_recv.at[k - 1],
            sem("trade", "s", k), sem("trade", "r", k), dp=target,
        )

    for cols in columns:
        part[0, :, cols] = (contract_rows(back_scaled, sav[:, cols]) * gain[:, cols].astype(F32)).astype(BF16)
        part[1, :, cols] = contract_rows(act_s, kept[:, cols]).astype(BF16)
    for k in range(1, n_dp):
        trade(k).start()

    if detour:
        for k in range(1, 4):
            helped, given, helper = side_way(k)

            @pl.when(helper)
            def _():
                helped.wait_recv()
                given.start()

    @pl.when(sec == 0)
    def _():
        next_in[...] = jnp.zeros_like(next_in)

    @pl.when(sec == n_sec - 1)
    def _():
        next_gr[...] = jnp.zeros_like(next_gr)

    def gather(p):
        held_rows = quarter << p
        block = pl.ds(pl.multiple_of(ten // (1 << p) * held_rows, held_rows), held_rows)
        return remote(pair.at[block], pair.at[block], sem("all", "s", p), sem("all", "r", p), tensor=flip(ten, p))

    @pl.when(sec > 0)
    def _():
        acts.wait_recv()

    @pl.when(sec < n_sec - 1)
    def _():
        backs.wait_recv()

    if bits:
        gather(0).start()

    for k in range(1, n_dp):
        trade(k).wait()
    for i, out in enumerate((grad_down, grad_up)):
        for cols in columns:
            summed = part[i, mine, cols].astype(F32)
            for k in range(1, n_dp):
                summed += part_recv[k - 1, i, :, cols].astype(F32)
            out[:, cols] = (summed * (1.0 / n_dp)).astype(BF16)

    for p in range(bits):
        gather(p).wait()
        if p + 1 < bits:
            gather(p + 1).start()
        if p == 0:
            pl.when(jnp.logical_and(sec > 0, dp % 2 == 1))(send_late)

    @pl.when(sec > 0)
    def _():
        for k in range(1, n_dp):
            relay(0, k).wait()
        raw_fwds.wait_recv()
        for a in range(0, raw_f, chunk):
            b = min(a + chunk, raw_f)
            grown = jnp.dot(pair[:, :rank], raw_up[:, a:b], preferred_element_type=F32)
            next_in[:, width - raw_f + a:width - raw_f + b] = (raw_fwd[:, a:b].astype(F32) + grown).astype(BF16)

    @pl.when(sec < n_sec - 1)
    def _():
        for k in range(1, n_dp):
            relay(1, k).wait()
        raw_pairs.wait_recv()
        far_tilt = jnp.sum(pair[:, padded + rank:].astype(F32), axis=1, keepdims=True)
        for a in range(0, raw_b, chunk):
            b = min(a + chunk, raw_b)
            normed = jnp.dot(pair[:, padded:padded + rank], raw_down[:, a:b], preferred_element_type=F32)
            next_gr[:, width - raw_b + a:width - raw_b + b] = (
                raw_pair[1, :, a:b].astype(F32)
                + normed
                - raw_pair[0, :, a:b].astype(F32) * far_tilt
            ).astype(BF16)

    if bits:
        remote(sq_in, sq_in, sem("sq", "s"), sem("sq", "r"), tensor=flip(ten, 0)).wait_send()
        remote(first_b, first_b, sem("first", "s"), sem("first", "r"), tensor=flip(ten, 0)).wait_send()
        if len(groups) > 1:
            rest = send_b.at[:, pl.ds(first_rows, rows - first_rows)]
            remote(rest, rest, sem("b_send"), sem("first", "r"), tensor=flip(ten, 0)).wait_send()
        remote(send_f, recv_f, sem("f_send"), sem("f", 0), tensor=flip(ten, 0)).wait_send()

    if detour:
        for k in range(1, 4):
            helped, given, helper = side_way(k)
            pl.when(helper)(given.wait_send)

    whole_f = across(1, fwd, out_f, sem("out_f", "s"), sem("out_f", "r"))
    whole_b = across(-1, kept, out_b, sem("out_b", "s"), sem("out_b", "r"))

    @pl.when(sec < n_sec - 1)
    def _():
        for copy in (raw_ups, acts, whole_f):
            copy.wait_send()

    @pl.when(sec > 0)
    def _():
        for copy in (raw_savs, raw_downs, backs, whole_b):
            copy.wait_send()

    @pl.when(sec < n_sec - 1)
    def _():
        shift(1, 0, rows, slice(0, width - raw_b)).wait_recv()

    @pl.when(sec > 0)
    def _():
        shift(0, 0, rows, slice(0, width - raw_f)).wait_recv()


def place(*refs):
    count = len(refs) // 2
    sems = refs[-1]
    copies = [pltpu.make_async_copy(refs[i], refs[count + i], sems.at[i]) for i in range(count)]
    for copy in copies:
        copy.start()
    for copy in copies:
        copy.wait()


def solution(mesh):
    n_sec, n_ten, n_dp = (mesh.shape[name] for name in ("section", "tensor", "dp"))

    def shards(forward_rows, saved_rows, output_grad, lengths, norm_gain, down_map, up_map):
        rows, width = forward_rows.shape[2:]
        rank = down_map.shape[1]
        n_seq = lengths.shape[2]
        share = rank // n_dp
        bits = n_ten.bit_length() - 1
        chunk = min(width, 4 * LANES)
        raw_f = int(width * RAW_FORWARD) // LANES * LANES
        raw_b = int(width * RAW_BACK) // LANES * LANES
        steps = max(bits, 1)
        padded = (rank + 3 + LANES - 1) // LANES * LANES
        vmem = pl.BlockSpec(memory_space=pltpu.VMEM)
        anywhere = pl.BlockSpec(memory_space=pl.ANY)
        flops = 7 * 2 * rows * rank * width
        dma = pltpu.SemaphoreType.DMA
        shapes = ((rows, width),) * 2 + ((share, width),) * 2
        results = pl.pallas_call(
            functools.partial(tick, (n_sec, n_ten, n_dp, chunk)),
            out_shape=tuple(pltpu.VMEM(shape, BF16) for shape in shapes),
            in_specs=[anywhere] * 7,
            out_specs=(vmem,) * 4,
            scratch_shapes=[
                pltpu.SMEM((1, n_seq), jnp.int32),
                pltpu.VMEM((1, width), BF16),
                pltpu.VMEM((rows, width), BF16),
                pltpu.VMEM((rows + rank, width), BF16),
                pltpu.VMEM((rows + rank, width), BF16),
                pltpu.VMEM((rows, width), BF16),
                pltpu.VMEM((rows, 2 * rank), F32),
                pltpu.VMEM((steps, rows, padded), BF16),
                pltpu.VMEM((steps, rows, padded), BF16),
                pltpu.VMEM((steps, rows, 2 * rank), BF16),
                pltpu.VMEM((steps, rows, 2 * rank), BF16),
                pltpu.VMEM((max(n_ten - 1, 1), row_groups(rows)[0][1], 2 * rank), BF16),
                pltpu.VMEM((rows, width), BF16),
                pltpu.VMEM((rows, width), BF16),
                pltpu.VMEM((2, rank, width), BF16),
                pltpu.VMEM((max(n_dp - 1, 1), 2, share, width), BF16),
                pltpu.VMEM((rows, padded), BF16),
                pltpu.VMEM((rows, padded), BF16),
                pltpu.VMEM((rows, 2 * padded), BF16),
                pltpu.VMEM((1, rows), F32),
                pltpu.VMEM((max(n_ten - 1, 1), 1, rows), F32),
                pltpu.VMEM((rows, raw_f), BF16),
                pltpu.VMEM((rank, raw_f), BF16),
                pltpu.VMEM((2, rows, raw_b), BF16),
                pltpu.VMEM((rank, raw_b), BF16),
                pltpu.VMEM((row_groups(rows)[1 % len(row_groups(rows))][1], 2 * LANES), BF16),
                dma((max(semaphores(len(row_groups(rows)), bits, n_dp).values()) + 1,)),
                pltpu.SemaphoreType.REGULAR,
                pltpu.SemaphoreType.REGULAR,
            ],
            compiler_params=pltpu.CompilerParams(collective_id=0, has_side_effects=True),
            cost_estimate=pl.CostEstimate(
                flops=flops, bytes_accessed=16 * rows * width, transcendentals=4 * rows * rank
            ),
            name="tick",
        )(
            forward_rows[0, 0], saved_rows[0, 0], output_grad[0, 0], lengths[0], norm_gain, down_map[0], up_map[0]
        )
        next_inputs, next_grads, grad_down, grad_up = pl.pallas_call(
            place,
            out_shape=tuple(jax.ShapeDtypeStruct(shape, BF16) for shape in shapes),
            in_specs=[vmem] * 4,
            out_specs=(anywhere,) * 4,
            scratch_shapes=[dma((4,))],
            name="place",
        )(*[pltpu.with_memory_space_constraint(x, pltpu.VMEM) for x in results])
        return next_inputs[None, None], next_grads[None, None], grad_down[None], grad_up[None]

    row_spec = P("section", "dp", None, "tensor")
    map_spec = P("section", None, "tensor")
    part_spec = P("section", "dp", "tensor")
    return jax.shard_map(
        shards,
        mesh=mesh,
        in_specs=(row_spec, row_spec, row_spec, P("section", "dp"), P("section", "tensor"), map_spec, map_spec),
        out_specs=(row_spec, row_spec, part_spec, part_spec),
        check_vma=False,
    )
```
